256 devices in a mesh: seq: 16 (over x, y_hi, core), batch: 16 (over y_lo, z).
Axes of the slice: x: 4, y: 4 (y_hi: 2, y_lo: 2; y = y_hi * 2 + y_lo), z: 8, core: 2. Of those that a mesh axis runs over, the one named last changes fastest.
Arguments:
- query_rows: bfloat16 [16, 2048, 2048], P('batch', 'seq'), may hold values from -6 to 6, as said below
- key_rows: bfloat16 [16, 2048, 1024], P('batch', 'seq'), may hold values from -6 to 6, as said below
- value_rows: bfloat16 [16, 2048, 1024], P('batch', 'seq'), may hold values from -6 to 6, as said below
- attn_output: bfloat16 [16, 2048, 2048], P('batch', 'seq'), may hold values from -6 to 6, as said below
- output_grad: bfloat16 [16, 2048, 2048], P('batch', 'seq'), may hold values from -6 to 6
- log_norm: float32 [16, 16, 2048], P('batch', None, 'seq'), as said below
- slab_order: int32 [16, 16], P('batch', 'seq'), may hold values from 0 to 15, as said below
- normed_input: bfloat16 [16, 2048, 4608], P('batch', 'seq'), may hold values from -6 to 6
Outputs:
- grad_query: bfloat16 [16, 2048, 2048], P('batch', 'seq')
- grad_key: bfloat16 [16, 2048, 1024], P('batch', 'seq')
- grad_weight: float32 [4608, 1024], P('seq')
The draws below stay inside these ranges and needn't reach their ends.
Inputs may be any that keep to these rules, and one draw needn't show every extreme that they name: `query_rows`: queries of a causal forward pass with 16 heads. `key_rows`: keys of the same forward pass with 8 heads. `value_rows`: values of the same forward pass. `attn_output`: the forward pass's output: for each head, sum over keys at or before the query's position of exp(score - log_norm) times the value. `log_norm`: log of the sum of exp(score) over the keys at or before the query's position, so that each row's weights sum to one. `slab_order`: each row is a permutation of the slab places.
All inputs are finite; a program needn't handle non-finite values.
Results may differ from the reference program's by a relative error of at most 0.025.
Values may be sent and summed in bfloat16 or wider, within the bound.
No kernel may reach another device: no remote copies, remote signals or barrier semaphores. Data moves between devices by JAX's collectives and lax.ppermute only.
A program may use at most 128 MiB of HBM per device.

```python
import jax
import jax.numpy as jnp
from jax import lax

D = 4608
HEADS = 16
KV_HEADS = 8
HEAD = 128
TOK_DEV = 128
LENGTH = 2048
BATCH = 16


SCALE = 144.0 ** (-0.5)


def slab_places(key):
    base = jax.random.fold_in(key, 11)
    subkeys = jax.random.split(base, BATCH)
    return jax.vmap(lambda subkey: jax.random.permutation(subkey, LENGTH // TOK_DEV))(subkeys).astype(jnp.int32)


def one_draw(subkey, width):
    values = jax.random.normal(subkey, (BATCH, LENGTH, width), jnp.float32)
    return jnp.clip(values, -6.0, 6.0).astype(jnp.bfloat16)


def projections(key):
    base = jax.random.fold_in(key, 23)
    first, second, third = jax.random.split(base, 3)
    return (one_draw(first, HEADS * HEAD), one_draw(second, KV_HEADS * HEAD), one_draw(third, KV_HEADS * HEAD))


def forward(key):
    queries, keys, values = projections(key)
    order = slab_places(key)
    group = HEADS // KV_HEADS

    def sequence(inputs):
        query_seq, key_seq, value_seq, order_row = inputs
        positions = (order_row[:, None] * TOK_DEV + jnp.arange(TOK_DEV, dtype=jnp.int32)[None, :]).reshape(LENGTH)
        query_f = query_seq.astype(jnp.float32).reshape(LENGTH, KV_HEADS, group, HEAD)
        key_f = key_seq.astype(jnp.float32).reshape(LENGTH, KV_HEADS, HEAD)
        value_f = value_seq.astype(jnp.float32).reshape(LENGTH, KV_HEADS, HEAD)
        scores = SCALE * jnp.einsum('tgrd,kgd->grtk', query_f, key_f)
        allowed = positions[None, :] <= positions[:, None]
        scores = jnp.where(allowed, scores, -1e+30)
        top = jnp.max(scores, axis=3, keepdims=True)
        weights = jnp.where(allowed, jnp.exp(scores - top), 0.0)
        total = jnp.sum(weights, axis=3, keepdims=True)
        outputs = jnp.einsum('grtk,kgd->tgrd', weights / total, value_f)
        norms = (top + jnp.log(total))[..., 0].reshape(HEADS, LENGTH)
        return (outputs.reshape(LENGTH, HEADS * HEAD).astype(jnp.bfloat16), norms)
    return lax.map(sequence, (queries, keys, values, order))


def draw_query_rows(key, part):
    return projections(key)[0]


def draw_key_rows(key, part):
    return projections(key)[1]


def draw_value_rows(key, part):
    return projections(key)[2]


def draw_attn_output(key, part):
    return forward(key)[0]


def draw_log_norm(key, part):
    return forward(key)[1]


def draw_slab_order(key, part):
    return slab_places(key)


def level_of(own_key, shape, shards, smallest, top_value):
    level = 1.0
    for dim, blocks in shards:
        heights = jax.random.uniform(jax.random.fold_in(jax.random.fold_in(own_key, 6), dim), (blocks,), jnp.float32, smallest / len(shards), top_value / len(shards))
        level = level * jnp.repeat(jnp.exp(heights), shape[dim] // blocks).reshape((-1,) + (1,) * (len(shape) - 1 - dim))
    return level


def scatter_about(stream_key, extent, scale, limit, shards=(), kind=jnp.bfloat16):
    drawn = jax.random.normal(stream_key, extent, jnp.float32) * scale
    if len(shards) > 0:
        drawn = level_of(stream_key, extent, shards, -0.22, 0.18) * drawn
    return jnp.clip(drawn, min=-limit, max=limit).astype(kind)


def setup_inputs(seed: int = 0) -> dict:
    seeds = jax.random.split(jax.random.key(seed), 9)
    return {
        "query_rows": draw_query_rows(jax.random.fold_in(seeds[8], 71), 0),
        "key_rows": draw_key_rows(jax.random.fold_in(seeds[8], 71), 0),
        "value_rows": draw_value_rows(jax.random.fold_in(seeds[8], 71), 0),
        "attn_output": draw_attn_output(jax.random.fold_in(seeds[8], 71), 0),
        "output_grad": scatter_about(seeds[4], (BATCH, LENGTH, HEADS * HEAD), 1.0, 6.0, ((0, 16), (1, 16))),
        "log_norm": draw_log_norm(jax.random.fold_in(seeds[8], 71), 0),
        "slab_order": draw_slab_order(jax.random.fold_in(seeds[8], 71), 0),
        "normed_input": scatter_about(seeds[7], (BATCH, LENGTH, D), 1.0, 6.0, ((0, 16), (1, 16))),
    }


SCALE = 144.0 ** -0.5


def rounded(values):
    return lax.optimization_barrier(values.astype(jnp.bfloat16)).astype(jnp.float32)


def block_terms(query_rows, output_rows, grad_rows, norm_rows, query_pos, key_rows, value_rows, key_pos):
    count = query_rows.shape[0]
    keys_count = key_rows.shape[0]
    group = HEADS // KV_HEADS
    queries = query_rows.astype(jnp.float32).reshape(count, KV_HEADS, group, HEAD)
    grads = grad_rows.astype(jnp.float32).reshape(count, KV_HEADS, group, HEAD)
    outputs = output_rows.astype(jnp.float32).reshape(count, KV_HEADS, group, HEAD)
    keys = key_rows.astype(jnp.float32).reshape(keys_count, KV_HEADS, HEAD)
    values = value_rows.astype(jnp.float32).reshape(keys_count, KV_HEADS, HEAD)
    norms = norm_rows.reshape(KV_HEADS, group, count)
    delta = jnp.transpose(jnp.sum(grads * outputs, axis=3), (1, 2, 0))
    scores = SCALE * jnp.einsum('tgrd,kgd->grtk', queries, keys)
    allowed = key_pos[None, :] <= query_pos[:, None]
    probs = jnp.where(allowed, jnp.exp(scores - norms[..., None]), 0.0)
    dprob = jnp.einsum('tgrd,kgd->grtk', grads, values)
    dscore = probs * (dprob - delta[..., None])
    probs_low = rounded(probs)
    dscore_low = rounded(dscore)
    grad_q = SCALE * jnp.einsum('grtk,kgd->tgrd', dscore_low, keys)
    grad_k = SCALE * jnp.einsum('grtk,tgrd->kgd', dscore_low, queries)
    grad_v = jnp.einsum('grtk,tgrd->kgd', probs_low, grads)
    return (grad_q.reshape(count, HEADS * HEAD),
            grad_k.reshape(keys_count, KV_HEADS * HEAD),
            grad_v.reshape(keys_count, KV_HEADS * HEAD))


def reference(query_rows, key_rows, value_rows, attn_output, output_grad, log_norm, slab_order, normed_input):
    slabs = LENGTH // TOK_DEV
    kv_width = KV_HEADS * HEAD

    def sequence(weight, inputs):
        queries, keys, values, outputs, grads, norms, order, normed = inputs
        positions = (order[:, None].astype(jnp.int32) * TOK_DEV
                     + jnp.arange(TOK_DEV, dtype=jnp.int32)[None, :]).reshape(LENGTH)

        def per_slab(carry, index):
            acc_key, acc_value = carry
            start = (index * TOK_DEV).astype(jnp.int32)
            grad_q, grad_k, grad_v = block_terms(
                lax.dynamic_slice_in_dim(queries, start, TOK_DEV, 0),
                lax.dynamic_slice_in_dim(outputs, start, TOK_DEV, 0),
                lax.dynamic_slice_in_dim(grads, start, TOK_DEV, 0),
                lax.dynamic_slice_in_dim(norms, start, TOK_DEV, 1),
                lax.dynamic_slice_in_dim(positions, start, TOK_DEV, 0),
                keys, values, positions)
            return (acc_key + rounded(grad_k), acc_value + rounded(grad_v)), grad_q.astype(jnp.bfloat16)

        zeros = jnp.zeros((LENGTH, kv_width), jnp.float32)
        (acc_key, acc_value), slab_query = lax.scan(per_slab, (zeros, zeros), jnp.arange(slabs, dtype=jnp.int32))
        grad_query = slab_query.reshape(LENGTH, HEADS * HEAD)
        grad_key = acc_key.astype(jnp.bfloat16)
        grad_value = acc_value.astype(jnp.bfloat16).astype(jnp.float32)

        def per_weight(total, index):
            start = (index * TOK_DEV).astype(jnp.int32)
            rows_in = lax.dynamic_slice_in_dim(normed, start, TOK_DEV, 0).astype(jnp.float32)
            rows_grad = lax.dynamic_slice_in_dim(grad_value, start, TOK_DEV, 0)
            part = jnp.dot(rows_in.T, rows_grad, preferred_element_type=jnp.float32)
            return total + rounded(part), None

        weight, _ = lax.scan(per_weight, weight, jnp.arange(slabs, dtype=jnp.int32))
        return weight, (grad_query, grad_key)

    start_weight = jnp.zeros((D, kv_width), jnp.float32)
    weight, (grad_query, grad_key) = lax.scan(
        sequence, start_weight,
        (query_rows, key_rows, value_rows, attn_output, output_grad, log_norm, slab_order, normed_input))
    return grad_query, grad_key, weight
```

```python
import jax
import jax.numpy as jnp
from jax import lax
from jax.experimental import pallas as pl
from jax.experimental.pallas import tpu as pltpu
from jax.sharding import PartitionSpec as P

HEADS = 16
KV_HEADS = 8
HEAD = 128
TOK = 128
SLABS = 16
LENGTH = 2048
CHIPS = 8
D = 4608
ROWS = D // SLABS
BK = 256
BQ = 512
PACK = 3 * TOK + 8
XW = 640

SCALE = 144.0 ** (-0.5)
LOG2E = 1.4426950408889634

f32 = jnp.float32
bf16 = jnp.bfloat16


def dot(a, b, dims):
    return lax.dot_general(a, b, (dims, ((), ())), preferred_element_type=f32)


def three_parts(x):
    hi = x.astype(bf16).astype(f32)
    rest = x - hi
    mid = rest.astype(bf16).astype(f32)
    low = (rest - mid).astype(bf16).astype(f32)
    return hi, mid, low


def pack_kernel(place_ref, q_ref, g_ref, o_ref, k_ref, v_ref, n_ref, out_ref):
    place = jnp.full((1, TOK), place_ref[0, 0], jnp.int32).astype(f32)
    for s in range(SLABS):
        cols = slice(s * HEAD, (s + 1) * HEAD)
        kv_cols = slice((s // 2) * HEAD, (s // 2 + 1) * HEAD)
        grads = g_ref[:, cols]
        out_ref[s, 0:TOK, :] = q_ref[:, cols]
        out_ref[s, TOK : 2 * TOK, :] = grads
        out_ref[s, 2 * TOK : 3 * TOK, :] = (k_ref if s % 2 == 0 else v_ref)[:, kv_cols]
        prod = grads.astype(f32) * o_ref[:, cols].astype(f32)
        delta = jnp.sum(prod.T, axis=0, keepdims=True)
        rows = (*three_parts(n_ref[s : s + 1, :]), *three_parts(delta), place, jnp.zeros_like(place))
        out_ref[s, 3 * TOK :, :] = jnp.concatenate(rows, axis=0).astype(bf16)


def attn_kernel(
    core_ref, in_ref, oth_ref, qk_ref, keep_ref, send_ref,
    q_s, g_s, k_s, v_s, nd_s, dq_s, dk_s, dv_s, inv_s,
):
    core = core_ref[0, 0]
    for s in range(SLABS):
        extra = in_ref[s, 3 * TOK :, :].astype(f32)
        p = jnp.max(extra[6:7, :]).astype(jnp.int32)
        inv_s[p] = s
        at = pl.ds(pl.multiple_of(p * TOK, TOK), TOK)
        q_s[at, :] = in_ref[s, 0:TOK, :]
        g_s[at, :] = in_ref[s, TOK : 2 * TOK, :]
        own = in_ref[s, 2 * TOK : 3 * TOK, :]
        oth = oth_ref[s]
        k_s[at, :] = jnp.where(core == 0, own, oth)
        v_s[at, :] = jnp.where(core == 0, oth, own)
        norm = (extra[0:1] + extra[1:2] + extra[2:3]) * LOG2E
        delta = extra[3:4] + extra[4:5] + extra[5:6]
        nd_s[p, 0:1, :] = norm
        nd_s[p, 1:2, :] = delta
    dq_s[...] = jnp.zeros_like(dq_s)

    def one(j, i, kb, kt, vb, masked):
        qb = q_s[pl.ds(pl.multiple_of(i * BQ, BQ), BQ), :]
        gb = g_s[pl.ds(pl.multiple_of(i * BQ, BQ), BQ), :]
        norm = jnp.concatenate([nd_s[i * (BQ // TOK) + t, 0:1, :] for t in range(BQ // TOK)], axis=1)
        delta = jnp.concatenate([nd_s[i * (BQ // TOK) + t, 1:2, :] for t in range(BQ // TOK)], axis=1)
        st = dot(kb, qb, ((1,), (1,)))
        probs = jnp.exp2(st * (SCALE * LOG2E) - norm)
        if masked:
            key_at = lax.broadcasted_iota(jnp.int32, (BK, BQ), 0) + j * BK
            query_at = lax.broadcasted_iota(jnp.int32, (BK, BQ), 1) + i * BQ
            probs = jnp.where(key_at <= query_at, probs, 0.0)
        dprob = dot(vb, gb, ((1,), (1,)))
        ds = (probs * (dprob - delta)).astype(bf16)
        dv = dot(probs.astype(bf16), gb, ((1,), (0,)))
        dk = dot(ds, qb, ((1,), (0,)))
        dq_s[i] += dot(kt, ds, ((1,), (0,)))
        return dk, dv

    def per_key_block(j, _):
        at = pl.ds(pl.multiple_of(j * BK, BK), BK)
        kb = k_s[at, :]
        vb = v_s[at, :]
        kt = kb.T
        first = j // (BQ // BK)
        dk, dv = one(j, first, kb, kt, vb, True)
        dk_s[...] = dk
        dv_s[...] = dv

        def per_query_block(i, _):
            dk, dv = one(j, i, kb, kt, vb, False)
            dk_s[...] += dk
            dv_s[...] += dv
            return 0

        lax.fori_loop(first + 1, LENGTH // BQ, per_query_block, 0)
        for t in range(BK // TOK):
            s = inv_s[j * (BK // TOK) + t]
            qk_ref[s, TOK:, :] = (dk_s[t * TOK : (t + 1) * TOK, :] * SCALE).astype(bf16)
            part = dv_s[t * TOK : (t + 1) * TOK, :]

            @pl.when(s % 2 == core)
            def _():
                keep_ref[s // 2] = part

            @pl.when(s % 2 != core)
            def _():
                send_ref[s // 2] = part.astype(bf16)

        return 0

    lax.fori_loop(0, LENGTH // BK, per_key_block, 0)
    for i in range(LENGTH // BQ):
        rows = (dq_s[i].T * SCALE).astype(bf16)
        for t in range(BQ // TOK):
            s = inv_s[i * (BQ // TOK) + t]
            qk_ref[s, 0:TOK, :] = rows[t * TOK : (t + 1) * TOK, :]


def weight_kernel(place_ref, xt_ref, dv_ref, keep_ref, send_ref):
    core = place_ref[0, 0]
    base = place_ref[0, 1]
    own = pl.multiple_of(base + core * ROWS, 32)
    other = pl.multiple_of(base + (1 - core) * ROWS, 32)
    grads = jnp.concatenate([dv_ref[0], dv_ref[1]], axis=1)
    mine = dot(xt_ref[pl.ds(own, ROWS), :], grads, ((1,), (0,)))
    sent = dot(xt_ref[pl.ds(other, ROWS), :], grads, ((1,), (0,))).astype(bf16)
    half = ROWS // 2
    for r in range(2):
        for h in range(2):
            keep_ref[r, h] = mine[r * half : (r + 1) * half, h * HEAD : (h + 1) * HEAD]
            send_ref[r, h] = sent[r * half : (r + 1) * half, h * HEAD : (h + 1) * HEAD]


VMEM = pl.BlockSpec(memory_space=pltpu.VMEM)
SMEM = pl.BlockSpec(memory_space=pltpu.SMEM)


def pack(place, q, g, o, k, v, n):
    return pl.pallas_call(
        pack_kernel,
        in_specs=[SMEM] + [VMEM] * 6,
        out_specs=VMEM,
        out_shape=jax.ShapeDtypeStruct((SLABS, PACK, HEAD), bf16),
        name="pack",
    )(place, q, g, o, k, v, n)


def attention(core, packed, other):
    half = (CHIPS, TOK, HEAD)
    return pl.pallas_call(
        attn_kernel,
        in_specs=[SMEM, VMEM, VMEM],
        out_specs=[VMEM] * 3,
        out_shape=[
            jax.ShapeDtypeStruct((SLABS, 2 * TOK, HEAD), bf16),
            jax.ShapeDtypeStruct(half, f32),
            jax.ShapeDtypeStruct(half, bf16),
        ],
        scratch_shapes=[pltpu.VMEM((LENGTH, HEAD), bf16)] * 4
        + [
            pltpu.VMEM((SLABS, 8, TOK), f32),
            pltpu.VMEM((LENGTH // BQ, HEAD, BQ), f32),
            pltpu.VMEM((BK, HEAD), f32),
            pltpu.VMEM((BK, HEAD), f32),
            pltpu.SMEM((SLABS,), jnp.int32),
        ],
        cost_estimate=pl.CostEstimate(flops=6 * 10**9, bytes_accessed=4 * 10**6, transcendentals=2 * 10**6),
        name="attention",
    )(core, packed, other)


def weight_rows(place, xt, dv):
    shape = (2, KV_HEADS, ROWS // 2, HEAD)
    block = pl.BlockSpec((2, 2, ROWS // 2, HEAD), lambda n: (0, n, 0, 0))
    return pl.pallas_call(
        weight_kernel,
        grid=(KV_HEADS // 2,),
        in_specs=[SMEM, VMEM, pl.BlockSpec((2, LENGTH // 2, HEAD), lambda n: (n, 0, 0))],
        out_specs=[block, block],
        out_shape=[jax.ShapeDtypeStruct(shape, f32), jax.ShapeDtypeStruct(shape, bf16)],
        cost_estimate=pl.CostEstimate(flops=2 * 10**9, bytes_accessed=5 * 10**6, transcendentals=0),
        name="weight",
    )(place, xt, dv)


SWAP = [(i, i ^ 1) for i in range(SLABS)]
SAME_CORE = [list(range(c, SLABS, 2)) for c in range(2)]


def local(
    query_rows, key_rows, value_rows, attn_output, output_grad, log_norm, slab_order, normed_input
):
    me = lax.axis_index("seq")
    core = me % 2
    packed = pack(
        slab_order, query_rows[0], output_grad[0], attn_output[0], key_rows[0], value_rows[0], log_norm[0]
    )
    got = lax.all_to_all(packed, "seq", 0, 0, tiled=True)
    other = lax.ppermute(got[:, 2 * TOK : 3 * TOK, :], "seq", SWAP)
    x = normed_input[0]
    starts = [1152 * (d // 2) + 512 * (d % 2) for d in range(CHIPS)]
    x_out = jnp.stack([x[:, a : a + XW] for a in starts])
    got, x_out = lax.optimization_barrier((got, x_out))
    x_in = lax.all_to_all(x_out, "seq", 0, 0, axis_index_groups=SAME_CORE, tiled=True)
    qk, keep, send = attention(core.reshape(1, 1), got, other)
    dv = (keep + lax.ppermute(send, "seq", SWAP).astype(f32)).astype(bf16)
    dv = dv.reshape(1, LENGTH // 2, HEAD)
    dv_all = lax.all_to_all(
        jnp.broadcast_to(dv, (CHIPS, LENGTH // 2, HEAD)), "seq", 0, 0, axis_index_groups=SAME_CORE, tiled=True
    )
    xt = x_in.reshape(LENGTH // 2, XW).T
    qk, dv_all = lax.optimization_barrier((qk, dv_all))
    qk_in = lax.all_to_all(qk, "seq", 0, 0, tiled=True)
    place = jnp.stack([core, (me // 2 % 2) * 64]).reshape(1, 2)
    w_keep, w_send = weight_rows(place, xt, dv_all)
    w = (w_keep + lax.ppermute(w_send, "seq", SWAP).astype(f32)).astype(bf16)
    parts = lax.all_to_all(w.reshape(SLABS, ROWS // 2, HEAD), "batch", 0, 0, tiled=True)
    piece = jnp.sum(parts.astype(f32), axis=0).astype(bf16)
    pieces = lax.all_to_all(
        jnp.broadcast_to(piece[None], (SLABS, ROWS // 2, HEAD)), "batch", 0, 0, tiled=True
    )
    weight = pieces.reshape(2, KV_HEADS, ROWS // 2, HEAD).transpose(0, 2, 1, 3).reshape(ROWS, KV_HEADS * HEAD)
    grad_query = qk_in[:, :TOK, :].transpose(1, 0, 2).reshape(1, TOK, HEADS * HEAD)
    pair = qk_in[:, TOK:, :].astype(f32).reshape(KV_HEADS, 2, TOK, HEAD)
    grad_key = (pair[:, 0] + pair[:, 1]).astype(bf16).transpose(1, 0, 2).reshape(1, TOK, KV_HEADS * HEAD)
    return (grad_query, grad_key, weight.astype(f32))


def solution(mesh):
    placed = (
        P("batch", "seq", None),
        P("batch", "seq", None),
        P("batch", "seq", None),
        P("batch", "seq", None),
        P("batch", "seq", None),
        P("batch", None, "seq"),
        P("batch", "seq"),
        P("batch", "seq", None),
    )
    return jax.shard_map(
        local,
        mesh=mesh,
        in_specs=placed,
        out_specs=(P("batch", "seq", None), P("batch", "seq", None), P("seq", None)),
        check_vma=False,
    )
```

```python
import jax
import jax.numpy as jnp
from jax import lax
from jax.experimental import pallas as pl
from jax.experimental.pallas import tpu as pltpu
from jax.sharding import PartitionSpec as P


HEADS = 16
KV_HEADS = 8
HEAD = 128
TOK = 128
SLABS = 16
LENGTH = 2048
CHIPS = 8
D = 4608
ROWS = D // SLABS
BK = 256
BQ = 512
HALF = TOK // 2
PACK = 2 * TOK + HALF + 8
TILES = 5

SCALE = 144.0 ** (-0.5)
LOG2E = 1.4426950408889634

f32 = jnp.float32
bf16 = jnp.bfloat16


def dot(a, b, dims):
    return lax.dot_general(a, b, (dims, ((), ())), preferred_element_type=f32)


def three_parts(x):
    hi = x.astype(bf16).astype(f32)
    rest = x - hi
    mid = rest.astype(bf16).astype(f32)
    low = (rest - mid).astype(bf16).astype(f32)
    return hi, mid, low


def pack_kernel(place_ref, q_ref, g_ref, o_ref, k_ref, n_ref, out_ref):
    place = jnp.full((1, TOK), place_ref[0, 0], jnp.int32).astype(f32)
    for s in range(SLABS):
        cols = slice(s * HEAD, (s + 1) * HEAD)
        kv_cols = slice((s // 2) * HEAD, (s // 2 + 1) * HEAD)
        half = slice((s % 2) * HALF, (s % 2 + 1) * HALF)
        grads = g_ref[:, cols]
        out_ref[s, 0:TOK, :] = q_ref[:, cols]
        out_ref[s, TOK : 2 * TOK, :] = grads
        out_ref[s, 2 * TOK : 2 * TOK + HALF, :] = k_ref[half, kv_cols]
        prod = grads.astype(f32) * o_ref[:, cols].astype(f32)
        delta = jnp.sum(prod.T, axis=0, keepdims=True)
        rows = (*three_parts(n_ref[s : s + 1, :]), *three_parts(delta), place, jnp.zeros_like(place))
        out_ref[s, 2 * TOK + HALF :, :] = jnp.concatenate(rows, axis=0).astype(bf16)


def pack_late_kernel(x_ref, v_ref, out_ref):
    for d in range(CHIPS):
        first = 9 * (d // 2) + 4 * (d % 2)
        for t in range(TILES):
            out_ref[d, t * TOK : (t + 1) * TOK, :] = x_ref[:, (first + t) * 128 : (first + t + 1) * 128]
        out_ref[d, TILES * TOK :, :] = v_ref[:, d * HEAD : (d + 1) * HEAD]


def sort_slabs(core, in_ref, oth_ref, q_s, g_s, k_s, nd_s, inv_s):
    for s in range(SLABS):
        extra = in_ref[s, 2 * TOK + HALF :, :].astype(f32)
        p = jnp.max(extra[6:7, :]).astype(jnp.int32)
        inv_s[p] = s
        at = pl.ds(pl.multiple_of(p * TOK, TOK), TOK)
        q_s[at, :] = in_ref[s, 0:TOK, :]
        g_s[at, :] = in_ref[s, TOK : 2 * TOK, :]
        own = in_ref[s, 2 * TOK : 2 * TOK + HALF, :]
        oth = oth_ref[s]
        k_s[pl.ds(pl.multiple_of(p * TOK, TOK), HALF), :] = jnp.where(core == 0, own, oth)
        k_s[pl.ds(pl.multiple_of(p * TOK + HALF, HALF), HALF), :] = jnp.where(core == 0, oth, own)
        nd_s[p, 0:1, :] = (extra[0:1] + extra[1:2] + extra[2:3]) * LOG2E
        nd_s[p, 1:2, :] = extra[3:4] + extra[4:5] + extra[5:6]


def row_of(nd_s, i, row):
    return jnp.concatenate([nd_s[i * (BQ // TOK) + t, row : row + 1, :] for t in range(BQ // TOK)], axis=1)


def block_at(i, size):
    return pl.ds(pl.multiple_of(i * size, size), size)


def probs_of(j, i, kb, qb, nd_s, masked):
    st = dot(kb, qb, ((1,), (1,)))
    probs = jnp.exp2(st * (SCALE * LOG2E) - row_of(nd_s, i, 0))
    if masked:
        key_at = lax.broadcasted_iota(jnp.int32, (BK, BQ), 0) + j * BK
        query_at = lax.broadcasted_iota(jnp.int32, (BK, BQ), 1) + i * BQ
        probs = jnp.where(key_at <= query_at, probs, 0.0)
    return probs


def value_kernel(where_ref, in_ref, oth_ref, keep_ref, send_ref, q_s, g_s, k_s, nd_s, dv_s, inv_s):
    core = where_ref[0, 0]
    sort_slabs(core, in_ref, oth_ref, q_s, g_s, k_s, nd_s, inv_s)

    def per_key_block(j, _):
        kb = k_s[block_at(j, BK), :]
        first = j // (BQ // BK)

        def one(i, masked):
            probs = probs_of(j, i, kb, q_s[block_at(i, BQ), :], nd_s, masked)
            return dot(probs.astype(bf16), g_s[block_at(i, BQ), :], ((1,), (0,)))

        dv_s[...] = one(first, True)

        def per_query_block(i, _):
            dv_s[...] += one(i, False)
            return 0

        lax.fori_loop(first + 1, LENGTH // BQ, per_query_block, 0)
        for t in range(BK // TOK):
            s = inv_s[j * (BK // TOK) + t]
            part = dv_s[t * TOK : (t + 1) * TOK, :]

            @pl.when(s % 2 == core)
            def _():
                keep_ref[s // 2] = part

            @pl.when(s % 2 != core)
            def _():
                send_ref[s // 2] = part.astype(bf16)

        return 0

    lax.fori_loop(0, LENGTH // BK, per_key_block, 0)


def score_kernel(
    where_ref, in_ref, oth_ref, v_ref, voth_ref, qkeep_ref, qsend_ref, kkeep_ref, ksend_ref,
    q_s, g_s, k_s, v_s, nd_s, dq_s, dk_s, inv_s,
):
    core = where_ref[0, 0]
    chip = where_ref[0, 1]
    sort_slabs(core, in_ref, oth_ref, q_s, g_s, k_s, nd_s, inv_s)
    for p in range(SLABS):
        s = inv_s[p]
        at = slice(p * TOK, (p + 1) * TOK)
        v_s[at, :] = jnp.where(s % 2 == core, v_ref[s // 2], voth_ref[s // 2])
    dq_s[...] = jnp.zeros_like(dq_s)

    def per_key_block(j, _):
        kb = k_s[block_at(j, BK), :]
        vb = v_s[block_at(j, BK), :]
        kt = kb.T
        first = j // (BQ // BK)

        def one(i, masked):
            qb = q_s[block_at(i, BQ), :]
            probs = probs_of(j, i, kb, qb, nd_s, masked)
            dprob = dot(vb, g_s[block_at(i, BQ), :], ((1,), (1,)))
            ds = (probs * (dprob - row_of(nd_s, i, 1))).astype(bf16)
            dq_s[i] += dot(kt, ds, ((1,), (0,)))
            return dot(ds, qb, ((1,), (0,)))

        dk_s[...] = one(first, True)

        def per_query_block(i, _):
            dk_s[...] += one(i, False)
            return 0

        lax.fori_loop(first + 1, LENGTH // BQ, per_query_block, 0)
        for t in range(BK // TOK):
            s = inv_s[j * (BK // TOK) + t]
            to = (s // 2) ^ chip
            part = dk_s[t * TOK : (t + 1) * TOK, :] * SCALE

            @pl.when(s % 2 == core)
            def _():
                kkeep_ref[to] = part

            @pl.when(s % 2 != core)
            def _():
                ksend_ref[to] = part.astype(bf16)

        return 0

    lax.fori_loop(0, LENGTH // BK, per_key_block, 0)
    for i in range(LENGTH // BQ):
        rows = (dq_s[i].T * SCALE).astype(bf16)
        for t in range(BQ // TOK):
            s = inv_s[i * (BQ // TOK) + t]
            to = (s // 2) ^ chip
            part = rows[t * TOK : (t + 1) * TOK, :]

            @pl.when(s % 2 == core)
            def _():
                qkeep_ref[to] = part

            @pl.when(s % 2 != core)
            def _():
                qsend_ref[to] = part


def spread_kernel(keep_ref, got_ref, out_ref):
    total = (keep_ref[...] + got_ref[...].astype(f32)).astype(bf16)
    for d in range(CHIPS):
        out_ref[d] = total


def turn_kernel(x_ref, out_ref):
    for i in range(CHIPS):
        for t in range(TILES):
            out_ref[t * 128 : (t + 1) * 128, i * TOK : (i + 1) * TOK] = x_ref[i, t * TOK : (t + 1) * TOK, :].T


def weight_kernel(where_ref, xt_ref, dv_ref, keep_ref, send_ref):
    core = where_ref[0, 0]
    base = (where_ref[0, 1] % 2) * 64
    own = pl.multiple_of(base + core * ROWS, 32)
    other = pl.multiple_of(base + (1 - core) * ROWS, 32)
    grads = jnp.concatenate([dv_ref[0], dv_ref[1]], axis=1)
    mine = dot(xt_ref[pl.ds(own, ROWS), :], grads, ((1,), (0,)))
    sent = dot(xt_ref[pl.ds(other, ROWS), :], grads, ((1,), (0,))).astype(bf16)
    half = ROWS // 2
    for r in range(2):
        for h in range(2):
            keep_ref[r, h] = mine[r * half : (r + 1) * half, h * HEAD : (h + 1) * HEAD]
            send_ref[r, h] = sent[r * half : (r + 1) * half, h * HEAD : (h + 1) * HEAD]


def join_kernel(q_ref, q_came_ref, k_ref, k_came_ref, *out_refs):
    for k in range(CHIPS):
        out_refs[k][0] = q_ref[k]
        out_refs[k][1] = q_came_ref[k]
        out_refs[k][2] = (k_ref[k] + k_came_ref[k].astype(f32)).astype(bf16)


def place_kernel(where_ref, *refs):
    core = where_ref[0, 0]
    chip = where_ref[0, 1]
    q_ref, k_ref = refs[CHIPS:]
    for k in range(CHIPS):
        part = refs[k]
        head = chip ^ k
        q_ref[:, block_at(2 * head + core, HEAD)] = part[0]
        q_ref[:, block_at(2 * head + 1 - core, HEAD)] = part[1]
        k_ref[:, block_at(head, HEAD)] = part[2]


VMEM = pl.BlockSpec(memory_space=pltpu.VMEM)
SMEM = pl.BlockSpec(memory_space=pltpu.SMEM)
TOKENS = (CHIPS, TOK, HEAD)


def shaped(shape, dtype):
    return jax.ShapeDtypeStruct(shape, dtype)


def call(kernel, specs, outs, scratch=(), flops=10**6, moved=10**6, **more):
    return pl.pallas_call(
        kernel,
        in_specs=specs,
        out_shape=outs,
        scratch_shapes=list(scratch),
        cost_estimate=pl.CostEstimate(flops=flops, bytes_accessed=moved, transcendentals=0),
        **({"out_specs": [VMEM] * len(outs)} | more),
    )


SORTED = [pltpu.VMEM((LENGTH, HEAD), bf16)] * 3
ROWED = [pltpu.VMEM((SLABS, 8, TOK), f32)]
PLACES = [pltpu.SMEM((SLABS,), jnp.int32)]
BLOCK = [pltpu.VMEM((BK, HEAD), f32)]
SWAP = [(i, i ^ 1) for i in range(SLABS)]
SAME_CORE = [list(range(c, SLABS, 2)) for c in range(2)]


def swapped(array):
    return lax.ppermute(array, "seq", SWAP)


def inner(
    query_rows, key_rows, value_rows, attn_output, output_grad, log_norm, slab_order, normed_input
):
    me = lax.axis_index("seq").astype(jnp.int32)
    where = jnp.stack([me & 1, me >> 1]).reshape(1, 2)
    (packed,) = call(
        pack_kernel, [SMEM] + [VMEM] * 5, [shaped((SLABS, PACK, HEAD), bf16)]
    )(slab_order, query_rows[0], output_grad[0], attn_output[0], key_rows[0], log_norm[0])
    got = lax.all_to_all(packed, "seq", 0, 0, tiled=True)
    (late,) = call(pack_late_kernel, [VMEM] * 2, [shaped((CHIPS, 768, 128), bf16)])(normed_input[0], value_rows[0])
    got, late = lax.optimization_barrier((got, late))
    other = swapped(got[:, 2 * TOK : 2 * TOK + HALF, :])
    late_in = lax.all_to_all(late, "seq", 0, 0, axis_index_groups=SAME_CORE, tiled=True)
    keep, send = call(
        value_kernel, [SMEM, VMEM, VMEM], [shaped(TOKENS, f32), shaped(TOKENS, bf16)],
        SORTED + ROWED + BLOCK + PLACES, flops=3 * 10**9,
    )(where, got, other)
    came = swapped(send)
    (dv,) = call(spread_kernel, [VMEM] * 2, [shaped((CHIPS, *TOKENS), bf16)])(keep, came)
    dv_all = lax.all_to_all(dv.reshape(CHIPS, LENGTH // 2, HEAD), "seq", 0, 0, axis_index_groups=SAME_CORE, tiled=True)
    v_in = late_in[:, TILES * TOK :, :]
    v_other = swapped(v_in)
    q_keep, q_send, k_keep, k_send = call(
        score_kernel, [SMEM] + [VMEM] * 4,
        [shaped(TOKENS, bf16), shaped(TOKENS, bf16), shaped(TOKENS, f32), shaped(TOKENS, bf16)],
        SORTED + [pltpu.VMEM((LENGTH, HEAD), bf16)] + ROWED
        + [pltpu.VMEM((LENGTH // BQ, HEAD, BQ), f32)] + BLOCK + PLACES,
        flops=5 * 10**9,
    )(where, got, other, v_in, v_other)
    q_came, k_came = swapped(jnp.stack([q_send, k_send]))
    (xt,) = call(turn_kernel, [VMEM], [shaped((TILES * 128, LENGTH // 2), bf16)], flops=10**9)(late_in)
    block = pl.BlockSpec((2, 2, ROWS // 2, HEAD), lambda n: (0, n, 0, 0))
    w_shape = (2, KV_HEADS, ROWS // 2, HEAD)
    w_keep, w_send = call(
        weight_kernel,
        [SMEM, VMEM, pl.BlockSpec((2, LENGTH // 2, HEAD), lambda n: (n, 0, 0))],
        [shaped(w_shape, f32), shaped(w_shape, bf16)], flops=2 * 10**9,
        grid=(KV_HEADS // 2,), out_specs=[block, block],
    )(where, xt, dv_all)
    w_came = swapped(w_send)
    w = (w_keep + w_came.astype(f32)).astype(bf16)
    w, q_keep, q_came, k_keep, k_came = lax.optimization_barrier((w, q_keep, q_came, k_keep, k_came))
    back = call(join_kernel, [VMEM] * 4, [shaped((3, TOK, HEAD), bf16)] * CHIPS)(
        q_keep, q_came, k_keep, k_came
    )
    parts = lax.all_to_all(w.reshape(SLABS, ROWS // 2, HEAD), "batch", 0, 0, tiled=True)
    pieces = [back[0]]
    for k in range(1, CHIPS):
        pieces.append(lax.ppermute(back[k], "seq", [(i, i ^ (2 * k)) for i in range(SLABS)]))
    piece = jnp.sum(parts.astype(f32), axis=0).astype(bf16)
    blocks = lax.all_to_all(
        jnp.broadcast_to(piece[None], (SLABS, ROWS // 2, HEAD)), "batch", 0, 0, tiled=True
    )
    weight = blocks.reshape(2, KV_HEADS, ROWS // 2, HEAD).transpose(0, 2, 1, 3).reshape(ROWS, KV_HEADS * HEAD)
    grad_query, grad_key = call(
        place_kernel, [SMEM] + [VMEM] * CHIPS,
        [shaped((TOK, HEADS * HEAD), bf16), shaped((TOK, KV_HEADS * HEAD), bf16)],
    )(where, *pieces)
    return (grad_query[None], grad_key[None], weight.astype(f32))


def solution(mesh):
    placed = (
        P("batch", "seq", None),
        P("batch", "seq", None),
        P("batch", "seq", None),
        P("batch", "seq", None),
        P("batch", "seq", None),
        P("batch", None, "seq"),
        P("batch", "seq"),
        P("batch", "seq", None),
    )
    return jax.shard_map(
        inner,
        mesh=mesh,
        in_specs=placed,
        out_specs=(P("batch", "seq", None), P("batch", "seq", None), P("seq", None)),
        check_vma=False,
    )
```

```python
import jax
import jax.numpy as jnp
from jax import lax
from jax.experimental import pallas as pl
from jax.experimental.pallas import tpu as pltpu
from jax.sharding import Mesh, PartitionSpec as P


HEADS = 16
KV_HEADS = 8
HEAD = 128
TOK = 128
SLABS = 16
LENGTH = 2048
CHIPS = 8
D = 4608
ROWS = D // SLABS
QUARTER = ROWS // 4
BK = 256
BQ = 512
HALF = TOK // 2
PACK = 2 * TOK + HALF + 8
TILES = 9
XS = 4

SCALE = 144.0 ** (-0.5)
LOG2E = 1.4426950408889634

f32 = jnp.float32
bf16 = jnp.bfloat16


def dot(a, b, dims):
    return lax.dot_general(a, b, (dims, ((), ())), preferred_element_type=f32)


def three_parts(x):
    hi = x.astype(bf16).astype(f32)
    rest = x - hi
    mid = rest.astype(bf16).astype(f32)
    low = (rest - mid).astype(bf16).astype(f32)
    return hi, mid, low


def pack_kernel(place_ref, where_ref, q_ref, g_ref, o_ref, k_ref, v_ref, n_ref, out_ref, v_out_ref):
    for x in range(XS):
        v_out_ref[x] = v_ref[:, block_at(2 * x + 1 - where_ref[0, 2], HEAD)]
    place = jnp.full((1, TOK), place_ref[0, 0], jnp.int32).astype(f32)
    for s in range(SLABS):
        cols = slice(s * HEAD, (s + 1) * HEAD)
        kv_cols = slice((s // 2) * HEAD, (s // 2 + 1) * HEAD)
        half = slice((s % 2) * HALF, (s % 2 + 1) * HALF)
        grads = g_ref[:, cols]
        out_ref[s, 0:TOK, :] = q_ref[:, cols]
        out_ref[s, TOK : 2 * TOK, :] = grads
        out_ref[s, 2 * TOK : 2 * TOK + HALF, :] = k_ref[half, kv_cols]
        prod = grads.astype(f32) * o_ref[:, cols].astype(f32)
        delta = jnp.sum(prod.T, axis=0, keepdims=True)
        rows = (*three_parts(n_ref[s : s + 1, :]), *three_parts(delta), place, jnp.zeros_like(place))
        out_ref[s, 2 * TOK + HALF :, :] = jnp.concatenate(rows, axis=0).astype(bf16)


def pack_late_kernel(where_ref, x_ref, v_ref, v_came_ref, out_ref):
    for x in range(XS):
        for t in range(TILES):
            tile = TILES * x + t
            out_ref[x, t * TOK : (t + 1) * TOK, :] = x_ref[:, tile * 128 : (tile + 1) * 128].T
        out_ref[x, TILES * TOK : (TILES + 1) * TOK, :] = v_ref[:, block_at(2 * x + where_ref[0, 2], HEAD)]
        out_ref[x, (TILES + 1) * TOK :, :] = v_came_ref[x]


def sort_slabs(core, in_ref, oth_ref, q_s, g_s, k_s, nd_s, inv_s):
    for s in range(SLABS):
        extra = in_ref[s, 2 * TOK + HALF :, :].astype(f32)
        p = jnp.max(extra[6:7, :]).astype(jnp.int32)
        inv_s[p] = s
        at = pl.ds(pl.multiple_of(p * TOK, TOK), TOK)
        q_s[at, :] = in_ref[s, 0:TOK, :]
        g_s[at, :] = in_ref[s, TOK : 2 * TOK, :]
        own = in_ref[s, 2 * TOK : 2 * TOK + HALF, :]
        oth = oth_ref[s]
        k_s[pl.ds(pl.multiple_of(p * TOK, TOK), HALF), :] = jnp.where(core == 0, own, oth)
        k_s[pl.ds(pl.multiple_of(p * TOK + HALF, HALF), HALF), :] = jnp.where(core == 0, oth, own)
        nd_s[p, 0:1, :] = (extra[0:1] + extra[1:2] + extra[2:3]) * LOG2E
        nd_s[p, 1:2, :] = extra[3:4] + extra[4:5] + extra[5:6]


def row_of(nd_s, i, row):
    return jnp.concatenate([nd_s[i * (BQ // TOK) + t, row : row + 1, :] for t in range(BQ // TOK)], axis=1)


def block_at(i, size):
    return pl.ds(pl.multiple_of(i * size, size), size)


def probs_of(j, i, kb, qb, nd_s, masked):
    st = dot(kb, qb, ((1,), (1,)))
    probs = jnp.exp2(st * (SCALE * LOG2E) - row_of(nd_s, i, 0))
    if masked:
        key_at = lax.broadcasted_iota(jnp.int32, (BK, BQ), 0) + j * BK
        query_at = lax.broadcasted_iota(jnp.int32, (BK, BQ), 1) + i * BQ
        probs = jnp.where(key_at <= query_at, probs, 0.0)
    return probs


def value_kernel(where_ref, in_ref, oth_ref, keep_ref, send_ref, q_s, g_s, k_s, nd_s, dv_s, inv_s):
    core = where_ref[0, 0]
    sort_slabs(core, in_ref, oth_ref, q_s, g_s, k_s, nd_s, inv_s)

    def per_key_block(j, _):
        kb = k_s[block_at(j, BK), :]
        first = j // (BQ // BK)

        def one(i, masked):
            probs = probs_of(j, i, kb, q_s[block_at(i, BQ), :], nd_s, masked)
            return dot(probs.astype(bf16), g_s[block_at(i, BQ), :], ((1,), (0,)))

        dv_s[...] = one(first, True)

        def per_query_block(i, _):
            dv_s[...] += one(i, False)
            return 0

        lax.fori_loop(first + 1, LENGTH // BQ, per_query_block, 0)
        for t in range(BK // TOK):
            s = inv_s[j * (BK // TOK) + t]
            part = dv_s[t * TOK : (t + 1) * TOK, :]

            @pl.when(s % 2 == core)
            def _():
                keep_ref[s // 2] = part

            @pl.when(s % 2 != core)
            def _():
                send_ref[s // 2] = part.astype(bf16)

        return 0

    lax.fori_loop(0, LENGTH // BK, per_key_block, 0)


def score_kernel(
    where_ref, in_ref, oth_ref, v_ref, voth_ref, qkeep_ref, kkeep_ref, send_ref,
    q_s, g_s, k_s, v_s, nd_s, dq_s, dk_s, inv_s,
):
    core = where_ref[0, 0]
    chip = where_ref[0, 1]
    sort_slabs(core, in_ref, oth_ref, q_s, g_s, k_s, nd_s, inv_s)
    for p in range(SLABS):
        s = inv_s[p]
        at = slice(p * TOK, (p + 1) * TOK)
        at_x = s // 4
        rows = block_at(((s // 2) ^ chip) & 1, TOK)
        v_s[at, :] = jnp.where(s % 2 == core, v_ref[at_x, rows, :], voth_ref[at_x, rows, :])
    dq_s[...] = jnp.zeros_like(dq_s)

    def per_key_block(j, _):
        kb = k_s[block_at(j, BK), :]
        vb = v_s[block_at(j, BK), :]
        kt = kb.T
        first = j // (BQ // BK)

        def one(i, masked):
            qb = q_s[block_at(i, BQ), :]
            probs = probs_of(j, i, kb, qb, nd_s, masked)
            dprob = dot(vb, g_s[block_at(i, BQ), :], ((1,), (1,)))
            ds = (probs * (dprob - row_of(nd_s, i, 1))).astype(bf16)
            dq_s[i] += dot(kt, ds, ((1,), (0,)))
            return dot(ds, qb, ((1,), (0,)))

        dk_s[...] = one(first, True)

        def per_query_block(i, _):
            dk_s[...] += one(i, False)
            return 0

        lax.fori_loop(first + 1, LENGTH // BQ, per_query_block, 0)
        for t in range(BK // TOK):
            s = inv_s[j * (BK // TOK) + t]
            to = (s // 2) ^ chip
            part = dk_s[t * TOK : (t + 1) * TOK, :] * SCALE

            @pl.when(s % 2 == core)
            def _():
                kkeep_ref[to] = part

            @pl.when(s % 2 != core)
            def _():
                send_ref[1, to] = part.astype(bf16)

        return 0

    lax.fori_loop(0, LENGTH // BK, per_key_block, 0)
    for i in range(LENGTH // BQ):
        rows = (dq_s[i].T * SCALE).astype(bf16)
        for t in range(BQ // TOK):
            s = inv_s[i * (BQ // TOK) + t]
            to = (s // 2) ^ chip
            part = rows[t * TOK : (t + 1) * TOK, :]

            @pl.when(s % 2 == core)
            def _():
                qkeep_ref[to] = part

            @pl.when(s % 2 != core)
            def _():
                send_ref[0, to] = part


def sum_kernel(keep_ref, came_ref, out_ref):
    out_ref[...] = (keep_ref[...] + came_ref[...].astype(f32)).astype(bf16)


def weight_kernel(where_ref, mine_ref, came_ref, *refs):
    core = where_ref[0, 0]
    high = where_ref[0, 2]
    at_x = where_ref[0, 3]
    dv_refs, (keep_ref, send_ref, grad_s) = refs[:XS], refs[XS:]
    for i in range(CHIPS):
        slab = 2 * (i % XS) + (high if i < XS else 1 - high)
        for k in range(XS):
            grad_s[i * TOK : (i + 1) * TOK, k * HEAD : (k + 1) * HEAD] = dv_refs[k][slab]
    grads = grad_s[...]

    def rows_of(part, c):
        at = pl.ds(pl.multiple_of(part * 2 * ROWS + c * ROWS, 32), ROWS)
        tokens = [mine_ref[i, at, :] for i in range(XS)] + [came_ref[i, at, :] for i in range(XS)]
        return dot(jnp.concatenate(tokens, axis=1), grads, ((1,), (0,)))

    for part in range(2):
        mine = rows_of(part, core)
        for k in range(XS):
            for r in range(4):
                keep_ref[r, at_x ^ k, part] = mine[r * QUARTER : (r + 1) * QUARTER, k * HEAD : (k + 1) * HEAD]
        sent = rows_of(part, 1 - core).astype(bf16)
        for k in range(XS):
            for r in range(4):
                send_ref[r, at_x ^ k, part] = sent[r * QUARTER : (r + 1) * QUARTER, k * HEAD : (k + 1) * HEAD]


def finish_kernel(in_ref, out_ref):
    for high in range(2):
        for b in range(SLABS):
            head = 2 * (b % XS) + high
            rows = slice((b // XS) * QUARTER, (b // XS + 1) * QUARTER)
            out_ref[rows, head * HEAD : (head + 1) * HEAD] = in_ref[high * SLABS + b].astype(f32)


def join_kernel(q_ref, k_ref, came_ref, *out_refs):
    for k in range(CHIPS):
        out_refs[k][0] = q_ref[k]
        out_refs[k][1] = came_ref[0, k]
        out_refs[k][2] = (k_ref[k] + came_ref[1, k].astype(f32)).astype(bf16)


def place_kernel(where_ref, *refs):
    core = where_ref[0, 0]
    chip = where_ref[0, 1]
    q_ref, k_ref = refs[CHIPS:]
    for k in range(CHIPS):
        part = refs[k]
        head = chip ^ k
        q_ref[:, block_at(2 * head + core, HEAD)] = part[0]
        q_ref[:, block_at(2 * head + 1 - core, HEAD)] = part[1]
        k_ref[:, block_at(head, HEAD)] = part[2]


VMEM = pl.BlockSpec(memory_space=pltpu.VMEM)
SMEM = pl.BlockSpec(memory_space=pltpu.SMEM)
TOKENS = (CHIPS, TOK, HEAD)


def shaped(shape, dtype):
    return jax.ShapeDtypeStruct(shape, dtype)


def call(kernel, specs, outs, scratch=(), flops=10**6, moved=10**6, **more):
    return pl.pallas_call(
        kernel,
        in_specs=specs,
        out_shape=outs,
        scratch_shapes=list(scratch),
        cost_estimate=pl.CostEstimate(flops=flops, bytes_accessed=moved, transcendentals=0),
        **({"out_specs": [VMEM] * len(outs)} | more),
    )


SORTED = [pltpu.VMEM((LENGTH, HEAD), bf16)] * 3
ROWED = [pltpu.VMEM((SLABS, 8, TOK), f32)]
PLACES = [pltpu.SMEM((SLABS,), jnp.int32)]
BLOCK = [pltpu.VMEM((BK, HEAD), f32)]
SEQ = ("x", "yh", "core")
SWAP = [(0, 1), (1, 0)]


def swapped(array, axis="core"):
    return lax.ppermute(array, axis, SWAP)


def inner(
    query_rows, key_rows, value_rows, attn_output, output_grad, log_norm, slab_order, normed_input
):
    core, high, at_x = (lax.axis_index(a).astype(jnp.int32) for a in ("core", "yh", "x"))
    where = jnp.stack([core, at_x * 2 + high, high, at_x]).reshape(1, 4)
    packed, v_high = call(
        pack_kernel, [SMEM] * 2 + [VMEM] * 6,
        [shaped((SLABS, PACK, HEAD), bf16), shaped((XS, TOK, HEAD), bf16)],
    )(slab_order, where, query_rows[0], output_grad[0], attn_output[0], key_rows[0], value_rows[0], log_norm[0])
    got = lax.all_to_all(packed, SEQ, 0, 0, tiled=True)
    v_came = swapped(v_high, "yh")
    (late,) = call(
        pack_late_kernel, [SMEM] + [VMEM] * 3, [shaped((XS, (TILES + 2) * TOK, 128), bf16)]
    )(where, normed_input[0], value_rows[0], v_came)
    got, late = lax.optimization_barrier((got, late))
    other = swapped(got[:, 2 * TOK : 2 * TOK + HALF, :])
    late_in = lax.all_to_all(late, "x", 0, 0, tiled=True)
    x_mine = late_in[:, : TILES * TOK, :]
    x_came = swapped(x_mine, "yh")
    keep, send = call(
        value_kernel, [SMEM, VMEM, VMEM], [shaped(TOKENS, f32), shaped(TOKENS, bf16)],
        SORTED + ROWED + BLOCK + PLACES, flops=3 * 10**9,
    )(where, got, other)
    came = swapped(send)
    (dv,) = call(sum_kernel, [VMEM] * 2, [shaped(TOKENS, bf16)])(keep, came)
    dvs = [dv]
    for k in range(1, XS):
        dvs.append(lax.ppermute(dv, "x", [(i, i ^ k) for i in range(XS)]))
    v_in = late_in[:, TILES * TOK :, :]
    v_other = swapped(v_in)
    q_keep, k_keep, qk_send = call(
        score_kernel, [SMEM] + [VMEM] * 4,
        [shaped(TOKENS, bf16), shaped(TOKENS, f32), shaped((2, *TOKENS), bf16)],
        SORTED + [pltpu.VMEM((LENGTH, HEAD), bf16)] + ROWED
        + [pltpu.VMEM((LENGTH // BQ, HEAD, BQ), f32)] + BLOCK + PLACES,
        flops=5 * 10**9,
    )(where, got, other, v_in, v_other)
    qk_came = swapped(qk_send)
    w_shape = (4, XS, 2, QUARTER, HEAD)
    w_keep, w_send = call(
        weight_kernel, [SMEM] + [VMEM] * (2 + XS),
        [shaped(w_shape, f32), shaped(w_shape, bf16)],
        [pltpu.VMEM((LENGTH // 2, XS * HEAD), bf16)], flops=2 * 10**9,
    )(where, x_mine, x_came, *dvs)
    w_came = swapped(w_send)
    w = (w_keep + w_came.astype(f32)).astype(bf16)
    w, q_keep, k_keep, qk_came = lax.optimization_barrier((w, q_keep, k_keep, qk_came))
    parts = lax.all_to_all(w.reshape(SLABS, 2 * QUARTER, HEAD), "batch", 0, 0, tiled=True)
    back = call(join_kernel, [VMEM] * 3, [shaped((3, TOK, HEAD), bf16)] * CHIPS)(
        q_keep, k_keep, qk_came
    )
    pieces = [back[0]]
    for k in range(1, CHIPS):
        pieces.append(lax.ppermute(back[k], SEQ, [(i, i ^ (2 * k)) for i in range(SLABS)]))
    piece = jnp.sum(parts.astype(f32), axis=0).astype(bf16).reshape(2, 1, QUARTER, HEAD)
    blocks = lax.all_to_all(
        jnp.broadcast_to(piece, (2, SLABS, QUARTER, HEAD)).reshape(2 * SLABS, QUARTER, HEAD),
        ("yh", "batch"), 0, 0, tiled=True,
    )
    grad_query, grad_key = call(
        place_kernel, [SMEM] + [VMEM] * CHIPS,
        [shaped((TOK, HEADS * HEAD), bf16), shaped((TOK, KV_HEADS * HEAD), bf16)],
    )(where, *pieces)
    (weight,) = call(finish_kernel, [VMEM], [shaped((ROWS, KV_HEADS * HEAD), f32)])(blocks)
    return (grad_query[None], grad_key[None], weight)


def solution(mesh):
    fine = Mesh(mesh.devices.reshape(4, 2, 2, 16), (*SEQ, "batch"))
    rows = P("batch", SEQ, None)
    return jax.shard_map(
        inner,
        mesh=fine,
        in_specs=(rows, rows, rows, rows, rows, P("batch", None, SEQ), P("batch", SEQ), rows),
        out_specs=(rows, rows, P(SEQ, None)),
        check_vma=False,
    )
```

```python
import jax
import jax.numpy as jnp
from jax import lax
from jax.experimental import pallas as pl
from jax.experimental.pallas import tpu as pltpu
from jax.sharding import Mesh, PartitionSpec as P


HEADS = 16
KV_HEADS = 8
HEAD = 128
TOK = 128
SLABS = 16
LENGTH = 2048
CHIPS = 8
D = 4608
ROWS = D // SLABS
QUARTER = ROWS // 4
BK = 256
BQ = 512
HALF = TOK // 2
PACK = 3 * TOK + 8
TILES = 9
XS = 4
EARLY = (0, 1, 3)

SCALE = 144.0 ** (-0.5)
LOG2E = 1.4426950408889634

f32 = jnp.float32
bf16 = jnp.bfloat16


def dot(a, b, dims):
    return lax.dot_general(a, b, (dims, ((), ())), preferred_element_type=f32)


def three_parts(x):
    hi = x.astype(bf16).astype(f32)
    rest = x - hi
    mid = rest.astype(bf16).astype(f32)
    low = (rest - mid).astype(bf16).astype(f32)
    return hi, mid, low


def pack_kernel(place_ref, q_ref, g_ref, o_ref, k_ref, v_ref, n_ref, out_ref):
    place = jnp.full((1, TOK), place_ref[0, 0], jnp.int32).astype(f32)
    for s in range(SLABS):
        cols = slice(s * HEAD, (s + 1) * HEAD)
        kv_cols = slice((s // 2) * HEAD, (s // 2 + 1) * HEAD)
        half = slice((s % 2) * HALF, (s % 2 + 1) * HALF)
        grads = g_ref[:, cols]
        out_ref[s, 0:TOK, :] = q_ref[:, cols]
        out_ref[s, TOK : 2 * TOK, :] = grads
        out_ref[s, 2 * TOK : 2 * TOK + HALF, :] = k_ref[half, kv_cols]
        out_ref[s, 2 * TOK + HALF : 3 * TOK, :] = v_ref[half, kv_cols]
        prod = grads.astype(f32) * o_ref[:, cols].astype(f32)
        delta = jnp.sum(prod.T, axis=0, keepdims=True)
        rows = (*three_parts(n_ref[s : s + 1, :]), *three_parts(delta), place, jnp.zeros_like(place))
        out_ref[s, 3 * TOK :, :] = jnp.concatenate(rows, axis=0).astype(bf16)


def pack_late_kernel(where_ref, x_ref, out_ref, early_ref):
    for x in range(XS):
        for t in range(TILES):
            tile = TILES * x + t
            out_ref[x, t * TOK : (t + 1) * TOK, :] = x_ref[:, tile * 128 : (tile + 1) * 128].T
    for j, k in enumerate(EARLY):
        early_ref[j] = out_ref[where_ref[0, 3] ^ k]


def sort_slabs(core, in_ref, oth_ref, q_s, g_s, k_s, v_s, nd_s, inv_s):
    for s in range(SLABS):
        extra = in_ref[s, 3 * TOK :, :].astype(f32)
        p = jnp.max(extra[6:7, :]).astype(jnp.int32)
        inv_s[p] = s
        at = pl.ds(pl.multiple_of(p * TOK, TOK), TOK)
        q_s[at, :] = in_ref[s, 0:TOK, :]
        g_s[at, :] = in_ref[s, TOK : 2 * TOK, :]
        low = pl.ds(pl.multiple_of(p * TOK, TOK), HALF)
        high = pl.ds(pl.multiple_of(p * TOK + HALF, HALF), HALF)
        for part, out in enumerate((k_s, v_s)):
            own = in_ref[s, 2 * TOK + part * HALF : 2 * TOK + (part + 1) * HALF, :]
            oth = oth_ref[s, part * HALF : (part + 1) * HALF, :]
            out[low, :] = jnp.where(core == 0, own, oth)
            out[high, :] = jnp.where(core == 0, oth, own)
        nd_s[p, 0:1, :] = (extra[0:1] + extra[1:2] + extra[2:3]) * LOG2E
        nd_s[p, 1:2, :] = extra[3:4] + extra[4:5] + extra[5:6]


def row_of(nd_s, i, row):
    return jnp.concatenate([nd_s[i * (BQ // TOK) + t, row : row + 1, :] for t in range(BQ // TOK)], axis=1)


def block_at(i, size):
    return pl.ds(pl.multiple_of(i * size, size), size)


def attn_kernel(
    where_ref, in_ref, oth_ref, vkeep_ref, vsend_ref, qkeep_ref, kkeep_ref, send_ref,
    q_s, g_s, k_s, v_s, nd_s, dq_s, dk_s, dv_s, inv_s,
):
    core = where_ref[0, 0]
    chip = where_ref[0, 1]
    sort_slabs(core, in_ref, oth_ref, q_s, g_s, k_s, v_s, nd_s, inv_s)
    dq_s[...] = jnp.zeros_like(dq_s)

    def per_key_block(j, _):
        kb = k_s[block_at(j, BK), :]
        vb = v_s[block_at(j, BK), :]
        kt = kb.T
        first = j // (BQ // BK)

        def one(i, masked):
            qb = q_s[block_at(i, BQ), :]
            gb = g_s[block_at(i, BQ), :]
            st = dot(kb, qb, ((1,), (1,)))
            probs = jnp.exp2(st * (SCALE * LOG2E) - row_of(nd_s, i, 0))
            if masked:
                key_at = lax.broadcasted_iota(jnp.int32, (BK, BQ), 0) + j * BK
                query_at = lax.broadcasted_iota(jnp.int32, (BK, BQ), 1) + i * BQ
                probs = jnp.where(key_at <= query_at, probs, 0.0)
            dprob = dot(vb, gb, ((1,), (1,)))
            ds = (probs * (dprob - row_of(nd_s, i, 1))).astype(bf16)
            dv = dot(probs.astype(bf16), gb, ((1,), (0,)))
            dk = dot(ds, qb, ((1,), (0,)))
            dq_s[i] += dot(kt, ds, ((1,), (0,)))
            return dk, dv

        dk_s[...], dv_s[...] = one(first, True)

        def per_query_block(i, _):
            dk, dv = one(i, False)
            dk_s[...] += dk
            dv_s[...] += dv
            return 0

        lax.fori_loop(first + 1, LENGTH // BQ, per_query_block, 0)
        for t in range(BK // TOK):
            s = inv_s[j * (BK // TOK) + t]
            to = (s // 2) ^ chip
            rows = slice(t * TOK, (t + 1) * TOK)

            @pl.when(s % 2 == core)
            def _():
                vkeep_ref[s // 2] = dv_s[rows, :]
                kkeep_ref[to] = dk_s[rows, :] * SCALE

            @pl.when(s % 2 != core)
            def _():
                vsend_ref[s // 2] = dv_s[rows, :].astype(bf16)
                send_ref[1, to] = (dk_s[rows, :] * SCALE).astype(bf16)

        return 0

    lax.fori_loop(0, LENGTH // BK, per_key_block, 0)
    for i in range(LENGTH // BQ):
        rows = (dq_s[i].T * SCALE).astype(bf16)
        for t in range(BQ // TOK):
            s = inv_s[i * (BQ // TOK) + t]
            to = (s // 2) ^ chip
            part = rows[t * TOK : (t + 1) * TOK, :]

            @pl.when(s % 2 == core)
            def _():
                qkeep_ref[to] = part

            @pl.when(s % 2 != core)
            def _():
                send_ref[0, to] = part


def sum_kernel(keep_ref, came_ref, out_ref):
    out_ref[...] = (keep_ref[...] + came_ref[...].astype(f32)).astype(bf16)


def weight_kernel(where_ref, mine_ref, early_ref, one_ref, two_ref, three_ref, *refs):
    core = where_ref[0, 0]
    high = where_ref[0, 2]
    at_x = where_ref[0, 3]
    dv_refs, (keep_ref, send_ref, grad_s) = refs[:XS], refs[XS:]
    for i in range(CHIPS):
        slab = 2 * i + high if i < XS else 2 * (at_x ^ (i - XS)) + 1 - high
        for k in range(XS):
            grad_s[i * TOK : (i + 1) * TOK, k * HEAD : (k + 1) * HEAD] = dv_refs[k][slab]
    grads = grad_s[...]

    def rows_of(part, c):
        at = pl.ds(pl.multiple_of(part * 2 * ROWS + c * ROWS, 32), ROWS)
        tokens = [mine_ref[i, at, :] for i in range(XS)]
        tokens += [early_ref[0, at, :]] + [ref[at, :] for ref in (one_ref, two_ref, three_ref)]
        return dot(jnp.concatenate(tokens, axis=1), grads, ((1,), (0,)))

    for part in range(2):
        mine = rows_of(part, core)
        for k in range(XS):
            for r in range(4):
                keep_ref[r, at_x ^ k, part] = mine[r * QUARTER : (r + 1) * QUARTER, k * HEAD : (k + 1) * HEAD]
        sent = rows_of(part, 1 - core).astype(bf16)
        for k in range(XS):
            for r in range(4):
                send_ref[r, at_x ^ k, part] = sent[r * QUARTER : (r + 1) * QUARTER, k * HEAD : (k + 1) * HEAD]


def finish_kernel(in_ref, out_ref):
    for high in range(2):
        for b in range(SLABS):
            head = 2 * (b % XS) + high
            rows = slice((b // XS) * QUARTER, (b // XS + 1) * QUARTER)
            out_ref[rows, head * HEAD : (head + 1) * HEAD] = in_ref[high * SLABS + b].astype(f32)


def join_kernel(q_ref, k_ref, came_ref, *out_refs):
    for k in range(CHIPS):
        out_refs[k][0] = q_ref[k]
        out_refs[k][1] = came_ref[0, k]
        out_refs[k][2] = (k_ref[k] + came_ref[1, k].astype(f32)).astype(bf16)


def place_query_kernel(where_ref, *refs):
    core = where_ref[0, 0]
    chip = where_ref[0, 1]
    for k in range(CHIPS):
        head = chip ^ k
        refs[CHIPS][:, block_at(2 * head + core, HEAD)] = refs[k][0]
        refs[CHIPS][:, block_at(2 * head + 1 - core, HEAD)] = refs[k][1]


def place_key_kernel(where_ref, *refs):
    for k in range(CHIPS):
        refs[CHIPS][:, block_at(where_ref[0, 1] ^ k, HEAD)] = refs[k][2]


VMEM = pl.BlockSpec(memory_space=pltpu.VMEM)
SMEM = pl.BlockSpec(memory_space=pltpu.SMEM)
TOKENS = (CHIPS, TOK, HEAD)


def shaped(shape, dtype):
    return jax.ShapeDtypeStruct(shape, dtype)


def call(kernel, specs, outs, scratch=(), flops=10**6, moved=10**6, **more):
    return pl.pallas_call(
        kernel,
        in_specs=specs,
        out_shape=outs,
        scratch_shapes=list(scratch),
        cost_estimate=pl.CostEstimate(flops=flops, bytes_accessed=moved, transcendentals=0),
        **({"out_specs": [VMEM] * len(outs)} | more),
    )


SORTED = [pltpu.VMEM((LENGTH, HEAD), bf16)] * 4
ROWED = [pltpu.VMEM((SLABS, 8, TOK), f32)]
PLACES = [pltpu.SMEM((SLABS,), jnp.int32)]
BLOCK = [pltpu.VMEM((BK, HEAD), f32)]
SEQ = ("x", "yh", "core")
SWAP = [(0, 1), (1, 0)]


def swapped(array, axis="core"):
    return lax.ppermute(array, axis, SWAP)


def along_x(array, k):
    return lax.ppermute(array, "x", [(i, i ^ k) for i in range(XS)])


def inner(
    query_rows, key_rows, value_rows, attn_output, output_grad, log_norm, slab_order, normed_input
):
    core, high, at_x = (lax.axis_index(a).astype(jnp.int32) for a in ("core", "yh", "x"))
    where = jnp.stack([core, at_x * 2 + high, high, at_x]).reshape(1, 4)
    (packed,) = call(pack_kernel, [SMEM] + [VMEM] * 6, [shaped((SLABS, PACK, HEAD), bf16)])(
        slab_order, query_rows[0], output_grad[0], attn_output[0], key_rows[0], value_rows[0], log_norm[0]
    )
    got = lax.all_to_all(packed, SEQ, 0, 0, tiled=True)
    late, early = call(
        pack_late_kernel, [SMEM, VMEM],
        [shaped((XS, TILES * TOK, 128), bf16), shaped((len(EARLY), TILES * TOK, 128), bf16)],
    )(where, normed_input[0])
    early = swapped(early, "yh")
    got, late = lax.optimization_barrier((got, late))
    other = swapped(got[:, 2 * TOK : 3 * TOK, :])
    late = lax.all_to_all(late, "x", 0, 0, tiled=True)
    v_keep, v_send, q_keep, k_keep, qk_send = call(
        attn_kernel, [SMEM, VMEM, VMEM],
        [shaped(TOKENS, f32), shaped(TOKENS, bf16), shaped(TOKENS, bf16), shaped(TOKENS, f32), shaped((2, *TOKENS), bf16)],
        SORTED + ROWED + [pltpu.VMEM((LENGTH // BQ, HEAD, BQ), f32)] + BLOCK * 2 + PLACES,
        flops=6 * 10**9,
    )(where, got, other)
    v_came = swapped(v_send)
    (dv,) = call(sum_kernel, [VMEM] * 2, [shaped(TOKENS, bf16)])(v_keep, v_came)
    dvs = [dv]
    for k in range(1, XS):
        dvs.append(along_x(dv, k))
    two = swapped(lax.dynamic_index_in_dim(late, at_x ^ 2, 0, False), "yh")
    one, three = along_x(early[1], 1), along_x(early[2], 3)
    qk_came = swapped(qk_send)
    w_shape = (4, XS, 2, QUARTER, HEAD)
    w_keep, w_send = call(
        weight_kernel, [SMEM] + [VMEM] * (5 + XS),
        [shaped(w_shape, f32), shaped(w_shape, bf16)],
        [pltpu.VMEM((LENGTH // 2, XS * HEAD), bf16)], flops=2 * 10**9,
    )(where, late, early, one, two, three, *dvs)
    w_came = swapped(w_send)
    w = (w_keep + w_came.astype(f32)).astype(bf16)
    parts = lax.all_to_all(w.reshape(SLABS, 2 * QUARTER, HEAD), "batch", 0, 0, tiled=True)
    back = call(join_kernel, [VMEM] * 3, [shaped((3, TOK, HEAD), bf16)] * CHIPS)(
        q_keep, k_keep, qk_came
    )
    pieces = [back[0]]
    for k in range(1, CHIPS):
        pieces.append(lax.ppermute(back[k], SEQ, [(i, i ^ (2 * k)) for i in range(SLABS)]))
    piece = jnp.sum(parts.astype(f32), axis=0).astype(bf16).reshape(2, 1, QUARTER, HEAD)
    blocks = lax.all_to_all(
        jnp.broadcast_to(piece, (2, SLABS, QUARTER, HEAD)).reshape(2 * SLABS, QUARTER, HEAD),
        ("yh", "batch"), 0, 0, tiled=True,
    )
    (grad_query,) = call(
        place_query_kernel, [SMEM] + [VMEM] * CHIPS, [shaped((TOK, HEADS * HEAD), bf16)]
    )(where, *pieces)
    (grad_key,) = call(
        place_key_kernel, [SMEM] + [VMEM] * CHIPS, [shaped((TOK, KV_HEADS * HEAD), bf16)]
    )(where, *pieces)
    (weight,) = call(finish_kernel, [VMEM], [shaped((ROWS, KV_HEADS * HEAD), f32)])(blocks)
    return (grad_query[None], grad_key[None], weight)


def solution(mesh):
    fine = Mesh(mesh.devices.reshape(4, 2, 2, 16), (*SEQ, "batch"))
    rows = P("batch", SEQ, None)
    return jax.shard_map(
        inner,
        mesh=fine,
        in_specs=(rows, rows, rows, rows, rows, P("batch", None, SEQ), P("batch", SEQ), rows),
        out_specs=(rows, rows, P(SEQ, None)),
        check_vma=False,
    )
```

```python
import jax
import jax.numpy as jnp
from jax import lax
from jax.experimental import pallas as pl
from jax.experimental.pallas import tpu as pltpu
from jax.sharding import Mesh, PartitionSpec as P


HEADS = 16
KV_HEADS = 8
HEAD = 128
TOK = 128
SLABS = 16
LENGTH = 2048
CHIPS = 8
D = 4608
ROWS = D // SLABS
QUARTER = ROWS // 4
BK = 512
BQ = 512
HALF = TOK // 2
PACK = 3 * TOK + 8
TILES = 9
XS = 4
EARLY = (0, 1, 3)

SCALE = 144.0 ** (-0.5)
LOG2E = 1.4426950408889634

f32 = jnp.float32
bf16 = jnp.bfloat16


def dot(a, b, dims):
    return lax.dot_general(a, b, (dims, ((), ())), preferred_element_type=f32)


def three_parts(x):
    hi = x.astype(bf16).astype(f32)
    rest = x - hi
    mid = rest.astype(bf16).astype(f32)
    low = (rest - mid).astype(bf16).astype(f32)
    return hi, mid, low


def pack_kernel(place_ref, q_ref, g_ref, o_ref, k_ref, v_ref, n_ref, out_ref):
    place = jnp.full((1, TOK), place_ref[0, 0], jnp.int32).astype(f32)
    for s in range(SLABS):
        cols = slice(s * HEAD, (s + 1) * HEAD)
        kv_cols = slice((s // 2) * HEAD, (s // 2 + 1) * HEAD)
        half = slice((s % 2) * HALF, (s % 2 + 1) * HALF)
        grads = g_ref[:, cols]
        out_ref[s, 0:TOK, :] = q_ref[:, cols]
        out_ref[s, TOK : 2 * TOK, :] = grads
        out_ref[s, 2 * TOK : 2 * TOK + HALF, :] = k_ref[half, kv_cols]
        out_ref[s, 2 * TOK + HALF : 3 * TOK, :] = v_ref[half, kv_cols]
        prod = grads.astype(f32) * o_ref[:, cols].astype(f32)
        delta = jnp.sum(prod.T, axis=0, keepdims=True)
        rows = (*three_parts(n_ref[s : s + 1, :]), *three_parts(delta), place, jnp.zeros_like(place))
        out_ref[s, 3 * TOK :, :] = jnp.concatenate(rows, axis=0).astype(bf16)


def pack_late_kernel(where_ref, x_ref, out_ref, early_ref):
    for x in range(XS):
        for t in range(TILES):
            tile = TILES * x + t
            out_ref[x, t * TOK : (t + 1) * TOK, :] = x_ref[:, tile * 128 : (tile + 1) * 128].T
    for j, k in enumerate(EARLY):
        early_ref[j] = out_ref[where_ref[0, 3] ^ k]


def sort_slabs(core, in_ref, oth_ref, q_s, g_s, k_s, v_s, nd_s, inv_s):
    places = [jnp.max(in_ref[s, 3 * TOK :, :].astype(f32)[6:7, :]).astype(jnp.int32) for s in range(SLABS)]
    for s, p in enumerate(places):
        extra = in_ref[s, 3 * TOK :, :].astype(f32)
        inv_s[p] = s
        at = pl.ds(pl.multiple_of(p * TOK, TOK), TOK)
        q_s[at, :] = in_ref[s, 0:TOK, :]
        g_s[at, :] = in_ref[s, TOK : 2 * TOK, :]
        low = pl.ds(pl.multiple_of(p * TOK, TOK), HALF)
        high = pl.ds(pl.multiple_of(p * TOK + HALF, HALF), HALF)
        for part, out in enumerate((k_s, v_s)):
            own = in_ref[s, 2 * TOK + part * HALF : 2 * TOK + (part + 1) * HALF, :]
            oth = oth_ref[s, part * HALF : (part + 1) * HALF, :]
            out[low, :] = jnp.where(core == 0, own, oth)
            out[high, :] = jnp.where(core == 0, oth, own)
        nd_s[p, 0:1, :] = (extra[0:1] + extra[1:2] + extra[2:3]) * LOG2E
        nd_s[p, 1:2, :] = extra[3:4] + extra[4:5] + extra[5:6]


def row_of(nd_s, i, row):
    return jnp.concatenate([nd_s[i * (BQ // TOK) + t, row : row + 1, :] for t in range(BQ // TOK)], axis=1)


def block_at(i, size):
    if isinstance(i, int):
        return pl.ds(i * size, size)
    return pl.ds(pl.multiple_of(i * size, size), size)


def attn_kernel(
    where_ref, in_ref, oth_ref, vkeep_ref, vsend_ref, qkeep_ref, kkeep_ref, send_ref,
    q_s, g_s, k_s, v_s, nd_s, dq_s, dk_s, dv_s, inv_s,
):
    core = where_ref[0, 0]
    chip = where_ref[0, 1]
    sort_slabs(core, in_ref, oth_ref, q_s, g_s, k_s, v_s, nd_s, inv_s)
    dq_s[...] = jnp.zeros_like(dq_s)

    def per_key_block(j):
        kb = k_s[block_at(j, BK), :]
        vb = v_s[block_at(j, BK), :]
        kt = kb.T
        first = j // (BQ // BK)

        def one(i, masked):
            qb = q_s[block_at(i, BQ), :]
            gb = g_s[block_at(i, BQ), :]
            st = dot(kb, qb, ((1,), (1,)))
            probs = jnp.exp2(st * (SCALE * LOG2E) - row_of(nd_s, i, 0))
            if masked:
                key_at = lax.broadcasted_iota(jnp.int32, (BK, BQ), 0) + j * BK
                query_at = lax.broadcasted_iota(jnp.int32, (BK, BQ), 1) + i * BQ
                probs = jnp.where(key_at <= query_at, probs, 0.0)
            dprob = dot(vb, gb, ((1,), (1,)))
            ds = (probs * (dprob - row_of(nd_s, i, 1))).astype(bf16)
            dv = dot(probs.astype(bf16), gb, ((1,), (0,)))
            dk = dot(ds, qb, ((1,), (0,)))
            dq_s[i] += dot(kt, ds, ((1,), (0,)))
            return dk, dv

        dk_s[...], dv_s[...] = one(first, True)

        def per_query_block(i):
            dk, dv = one(i, False)
            dk_s[...] += dk
            dv_s[...] += dv
            return 0

        for i in range(first + 1, LENGTH // BQ):
            per_query_block(i)
        for t in range(BK // TOK):
            s = inv_s[j * (BK // TOK) + t]
            to = (s // 2) ^ chip
            rows = slice(t * TOK, (t + 1) * TOK)

            @pl.when(s % 2 == core)
            def _():
                vkeep_ref[s // 2] = dv_s[rows, :].astype(bf16)
                kkeep_ref[to] = (dk_s[rows, :] * SCALE).astype(bf16)

            @pl.when(s % 2 != core)
            def _():
                vsend_ref[s // 2] = dv_s[rows, :].astype(bf16)
                send_ref[1, to] = (dk_s[rows, :] * SCALE).astype(bf16)

        return 0

    for j in range(LENGTH // BK):
        per_key_block(j)
    for i in range(LENGTH // BQ):
        rows = (dq_s[i].T * SCALE).astype(bf16)
        for t in range(BQ // TOK):
            s = inv_s[i * (BQ // TOK) + t]
            to = (s // 2) ^ chip
            part = rows[t * TOK : (t + 1) * TOK, :]

            @pl.when(s % 2 == core)
            def _():
                qkeep_ref[to] = part

            @pl.when(s % 2 != core)
            def _():
                send_ref[0, to] = part


def weight_kernel(where_ref, mine_ref, early_ref, one_ref, two_ref, three_ref, *refs):
    core = where_ref[0, 0]
    high = where_ref[0, 2]
    at_x = where_ref[0, 3]
    dv_refs, (keep_ref, send_ref, grad_s) = refs[:XS], refs[XS:]
    for i in range(CHIPS):
        slab = 2 * i + high if i < XS else 2 * (at_x ^ (i - XS)) + 1 - high
        for k in range(XS):
            grad_s[i * TOK : (i + 1) * TOK, k * HEAD : (k + 1) * HEAD] = dv_refs[k][slab]
    grads = grad_s[...]

    def rows_of(part, c):
        at = pl.ds(pl.multiple_of(part * 2 * ROWS + c * ROWS, 32), ROWS)
        tokens = [mine_ref[i, at, :] for i in range(XS)]
        tokens += [early_ref[0, at, :]] + [ref[at, :] for ref in (one_ref, two_ref, three_ref)]
        return dot(jnp.concatenate(tokens, axis=1), grads, ((1,), (0,)))

    for part in range(2):
        mine = rows_of(part, core).astype(bf16)
        for k in range(XS):
            for r in range(4):
                keep_ref[r, at_x ^ k, part] = mine[r * QUARTER : (r + 1) * QUARTER, k * HEAD : (k + 1) * HEAD]
        sent = rows_of(part, 1 - core).astype(bf16)
        for k in range(XS):
            for r in range(4):
                send_ref[r, at_x ^ k, part] = sent[r * QUARTER : (r + 1) * QUARTER, k * HEAD : (k + 1) * HEAD]


def join_kernel(q_ref, k_ref, came_ref, *out_refs):
    for k in range(CHIPS):
        out_refs[k][0] = q_ref[k]
        out_refs[k][1] = came_ref[0, k]
        out_refs[k][2] = (k_ref[k].astype(f32) + came_ref[1, k].astype(f32)).astype(bf16)


def place_query_kernel(where_ref, *refs):
    core = where_ref[0, 0]
    chip = where_ref[0, 1]
    for k in range(CHIPS):
        head = chip ^ k
        refs[CHIPS][:, block_at(2 * head + core, HEAD)] = refs[k][0]
        refs[CHIPS][:, block_at(2 * head + 1 - core, HEAD)] = refs[k][1]


def place_key_kernel(where_ref, *refs):
    for k in range(CHIPS):
        refs[CHIPS][:, block_at(where_ref[0, 1] ^ k, HEAD)] = refs[k][2]


VMEM = pl.BlockSpec(memory_space=pltpu.VMEM)
SMEM = pl.BlockSpec(memory_space=pltpu.SMEM)
TOKENS = (CHIPS, TOK, HEAD)


def shaped(shape, dtype):
    return jax.ShapeDtypeStruct(shape, dtype)


def call(kernel, specs, outs, scratch=(), flops=10**6, moved=10**6, **more):
    return pl.pallas_call(
        kernel,
        in_specs=specs,
        out_shape=outs,
        scratch_shapes=list(scratch),
        cost_estimate=pl.CostEstimate(flops=flops, bytes_accessed=moved, transcendentals=0),
        **({"out_specs": [VMEM] * len(outs)} | more),
    )


SORTED = [pltpu.VMEM((LENGTH, HEAD), bf16)] * 4
ROWED = [pltpu.VMEM((SLABS, 8, TOK), f32)]
PLACES = [pltpu.SMEM((SLABS,), jnp.int32)]
BLOCK = [pltpu.VMEM((BK, HEAD), f32)]
SEQ = ("x", "yh", "core")
SWAP = [(0, 1), (1, 0)]


def swapped(array, axis="core"):
    return lax.ppermute(array, axis, SWAP)


def along_x(array, k):
    return lax.ppermute(array, "x", [(i, i ^ k) for i in range(XS)])


def inner(
    query_rows, key_rows, value_rows, attn_output, output_grad, log_norm, slab_order, normed_input
):
    core, high, at_x = (lax.axis_index(a).astype(jnp.int32) for a in ("core", "yh", "x"))
    where = jnp.stack([core, at_x * 2 + high, high, at_x]).reshape(1, 4)
    (packed,) = call(pack_kernel, [SMEM] + [VMEM] * 6, [shaped((SLABS, PACK, HEAD), bf16)])(
        slab_order, query_rows[0], output_grad[0], attn_output[0], key_rows[0], value_rows[0], log_norm[0]
    )
    got = lax.all_to_all(packed, SEQ, 0, 0, tiled=True)
    late, early = call(
        pack_late_kernel, [SMEM, VMEM],
        [shaped((XS, TILES * TOK, 128), bf16), shaped((len(EARLY), TILES * TOK, 128), bf16)],
    )(where, normed_input[0])
    early = swapped(early, "yh")
    got, late = lax.optimization_barrier((got, late))
    other = swapped(got[:, 2 * TOK : 3 * TOK, :])
    late = lax.all_to_all(late, "x", 0, 0, tiled=True)
    v_keep, v_send, q_keep, k_keep, qk_send = call(
        attn_kernel, [SMEM, VMEM, VMEM],
        [shaped(TOKENS, bf16)] * 4 + [shaped((2, *TOKENS), bf16)],
        SORTED + ROWED + [pltpu.VMEM((LENGTH // BQ, HEAD, BQ), f32)] + BLOCK * 2 + PLACES,
        flops=6 * 10**9,
    )(where, got, other)
    v_came = swapped(v_send)
    dv = (v_keep.astype(f32) + v_came.astype(f32)).astype(bf16)
    early, dv = lax.optimization_barrier((early, dv))
    dvs = [dv]
    for k in range(1, XS):
        dvs.append(along_x(dv, k))
    two = swapped(lax.dynamic_index_in_dim(late, at_x ^ 2, 0, False), "yh")
    one, three = along_x(early[1], 1), along_x(early[2], 3)
    qk_came = swapped(qk_send)
    w_shape = (4, XS, 2, QUARTER, HEAD)
    w_keep, w_send = call(
        weight_kernel, [SMEM] + [VMEM] * (5 + XS),
        [shaped(w_shape, bf16)] * 2,
        [pltpu.VMEM((LENGTH // 2, XS * HEAD), bf16)], flops=2 * 10**9,
    )(where, late, early, one, two, three, *dvs)
    w_came = swapped(w_send)
    w = (w_keep.astype(f32) + w_came.astype(f32)).astype(bf16)
    parts = lax.all_to_all(w.reshape(SLABS, 2 * QUARTER, HEAD), "batch", 0, 0, tiled=True)
    back = call(join_kernel, [VMEM] * 3, [shaped((3, TOK, HEAD), bf16)] * CHIPS)(
        q_keep, k_keep, qk_came
    )
    pieces = [back[0]]
    for k in range(1, CHIPS):
        pieces.append(lax.ppermute(back[k], SEQ, [(i, i ^ (2 * k)) for i in range(SLABS)]))
    piece = jnp.sum(parts.astype(f32), axis=0).astype(bf16).reshape(2, 1, QUARTER, HEAD)
    blocks = lax.all_to_all(
        jnp.broadcast_to(piece, (2, SLABS, QUARTER, HEAD)).reshape(2 * SLABS, QUARTER, HEAD),
        ("yh", "batch"), 0, 0, tiled=True,
    )
    (grad_query,) = call(
        place_query_kernel, [SMEM] + [VMEM] * CHIPS, [shaped((TOK, HEADS * HEAD), bf16)]
    )(where, *pieces)
    (grad_key,) = call(
        place_key_kernel, [SMEM] + [VMEM] * CHIPS, [shaped((TOK, KV_HEADS * HEAD), bf16)]
    )(where, *pieces)
    weight = blocks.reshape(2, 4, XS, QUARTER, HEAD).transpose(1, 3, 2, 0, 4).reshape(ROWS, KV_HEADS * HEAD)
    return (grad_query[None], grad_key[None], weight.astype(f32))


def solution(mesh):
    fine = Mesh(mesh.devices.reshape(4, 2, 2, 16), (*SEQ, "batch"))
    rows = P("batch", SEQ, None)
    return jax.shard_map(
        inner,
        mesh=fine,
        in_specs=(rows, rows, rows, rows, rows, P("batch", None, SEQ), P("batch", SEQ), rows),
        out_specs=(rows, rows, P(SEQ, None)),
        check_vma=False,
    )
```

```python
import jax
import jax.numpy as jnp
from jax import lax
from jax.experimental import pallas as pl
from jax.experimental.pallas import tpu as pltpu
from jax.sharding import Mesh, PartitionSpec as P


HEADS = 16
KV_HEADS = 8
HEAD = 128
TOK = 128
SLABS = 16
LENGTH = 2048
CHIPS = 8
D = 4608
ROWS = D // SLABS
QUARTER = ROWS // 4
BK = 512
BQ = 512
HALF = TOK // 2
PACK = 3 * TOK + 8
TILES = 9
PACKED = 4
XS = 4
EARLY = (0, 1, 3)

SCALE = 144.0 ** (-0.5)
LOG2E = 1.4426950408889634

f32 = jnp.float32
bf16 = jnp.bfloat16


def dot(a, b, dims):
    return lax.dot_general(a, b, (dims, ((), ())), preferred_element_type=f32)


def three_parts(x):
    hi = x.astype(bf16).astype(f32)
    rest = x - hi
    mid = rest.astype(bf16).astype(f32)
    low = (rest - mid).astype(bf16).astype(f32)
    return hi, mid, low


def pack_kernel(place_ref, q_ref, g_ref, o_ref, k_ref, v_ref, n_ref, out_ref):
    place = jnp.full((1, TOK), place_ref[0, 0], jnp.int32).astype(f32)
    for s in range(PACKED):
        cols = slice(s * HEAD, (s + 1) * HEAD)
        kv_cols = slice((s // 2) * HEAD, (s // 2 + 1) * HEAD)
        half = slice((s % 2) * HALF, (s % 2 + 1) * HALF)
        grads = g_ref[:, cols]
        out_ref[s, 0:TOK, :] = q_ref[:, cols]
        out_ref[s, TOK : 2 * TOK, :] = grads
        out_ref[s, 2 * TOK : 2 * TOK + HALF, :] = k_ref[half, kv_cols]
        out_ref[s, 2 * TOK + HALF : 3 * TOK, :] = v_ref[half, kv_cols]
        prod = grads.astype(f32) * o_ref[:, cols].astype(f32)
        delta = jnp.sum(prod.T, axis=0, keepdims=True)
        norm = n_ref[pl.ds(pl.program_id(0) * PACKED + s, 1), :]
        rows = (*three_parts(norm), *three_parts(delta), place, jnp.zeros_like(place))
        out_ref[s, 3 * TOK :, :] = jnp.concatenate(rows, axis=0).astype(bf16)


def pack_early_kernel(where_ref, x_ref, out_ref):
    for j, k in enumerate(EARLY):
        for t in range(TILES):
            tile = (where_ref[0, 3] ^ k) * TILES + t
            out_ref[j, t * TOK : (t + 1) * TOK, :] = x_ref[:, block_at(tile, 128)].T


def pack_late_kernel(x_ref, out_ref):
    for x in range(XS):
        for t in range(TILES):
            tile = TILES * x + t
            out_ref[x, t * TOK : (t + 1) * TOK, :] = x_ref[:, tile * 128 : (tile + 1) * 128].T


def sort_slabs(core, in_ref, oth_ref, q_s, g_s, k_s, v_s, nd_s, inv_s):
    places = [jnp.max(in_ref[s, 3 * TOK :, :].astype(f32)[6:7, :]).astype(jnp.int32) for s in range(SLABS)]
    for s, p in enumerate(places):
        extra = in_ref[s, 3 * TOK :, :].astype(f32)
        inv_s[p] = s
        at = pl.ds(pl.multiple_of(p * TOK, TOK), TOK)
        q_s[at, :] = in_ref[s, 0:TOK, :]
        g_s[at, :] = in_ref[s, TOK : 2 * TOK, :]
        low = pl.ds(pl.multiple_of(p * TOK, TOK), HALF)
        high = pl.ds(pl.multiple_of(p * TOK + HALF, HALF), HALF)
        for part, out in enumerate((k_s, v_s)):
            own = in_ref[s, 2 * TOK + part * HALF : 2 * TOK + (part + 1) * HALF, :]
            oth = oth_ref[s, part * HALF : (part + 1) * HALF, :]
            out[low, :] = jnp.where(core == 0, own, oth)
            out[high, :] = jnp.where(core == 0, oth, own)
        nd_s[p, 0:1, :] = (extra[0:1] + extra[1:2] + extra[2:3]) * LOG2E
        nd_s[p, 1:2, :] = extra[3:4] + extra[4:5] + extra[5:6]


def row_of(nd_s, i, row):
    return jnp.concatenate([nd_s[i * (BQ // TOK) + t, row : row + 1, :] for t in range(BQ // TOK)], axis=1)


def block_at(i, size):
    if isinstance(i, int):
        return pl.ds(i * size, size)
    return pl.ds(pl.multiple_of(i * size, size), size)


def attn_kernel(
    where_ref, in_ref, oth_ref, vkeep_ref, vsend_ref, qkeep_ref, kkeep_ref, send_ref,
    q_s, g_s, k_s, v_s, nd_s, dq_s, dk_s, dv_s, inv_s,
):
    core = where_ref[0, 0]
    chip = where_ref[0, 1]
    sort_slabs(core, in_ref, oth_ref, q_s, g_s, k_s, v_s, nd_s, inv_s)
    dq_s[...] = jnp.zeros_like(dq_s)

    def per_key_block(j):
        kb = k_s[block_at(j, BK), :]
        vb = v_s[block_at(j, BK), :]
        kt = kb.T
        first = j // (BQ // BK)

        def one(i, masked):
            qb = q_s[block_at(i, BQ), :]
            gb = g_s[block_at(i, BQ), :]
            st = dot(kb, qb, ((1,), (1,)))
            probs = jnp.exp2(st * (SCALE * LOG2E) - row_of(nd_s, i, 0))
            if masked:
                key_at = lax.broadcasted_iota(jnp.int32, (BK, BQ), 0) + j * BK
                query_at = lax.broadcasted_iota(jnp.int32, (BK, BQ), 1) + i * BQ
                probs = jnp.where(key_at <= query_at, probs, 0.0)
            dprob = dot(vb, gb, ((1,), (1,)))
            ds = (probs * (dprob - row_of(nd_s, i, 1))).astype(bf16)
            dv = dot(probs.astype(bf16), gb, ((1,), (0,)))
            dk = dot(ds, qb, ((1,), (0,)))
            dq_s[i] += dot(kt, ds, ((1,), (0,)))
            return dk, dv

        dk_s[...], dv_s[...] = one(first, True)

        def per_query_block(i):
            dk, dv = one(i, False)
            dk_s[...] += dk
            dv_s[...] += dv
            return 0

        for i in range(first + 1, LENGTH // BQ):
            per_query_block(i)
        for t in range(BK // TOK):
            s = inv_s[j * (BK // TOK) + t]
            to = (s // 2) ^ chip
            rows = slice(t * TOK, (t + 1) * TOK)

            @pl.when(s % 2 == core)
            def _():
                vkeep_ref[s // 2] = dv_s[rows, :].astype(bf16)
                kkeep_ref[to] = (dk_s[rows, :] * SCALE).astype(bf16)

            @pl.when(s % 2 != core)
            def _():
                vsend_ref[s // 2] = dv_s[rows, :].astype(bf16)
                send_ref[1, to] = (dk_s[rows, :] * SCALE).astype(bf16)

        return 0

    for j in range(LENGTH // BK):
        per_key_block(j)
    for i in range(LENGTH // BQ):
        rows = (dq_s[i].T * SCALE).astype(bf16)
        for t in range(BQ // TOK):
            s = inv_s[i * (BQ // TOK) + t]
            to = (s // 2) ^ chip
            part = rows[t * TOK : (t + 1) * TOK, :]

            @pl.when(s % 2 == core)
            def _():
                qkeep_ref[to] = part

            @pl.when(s % 2 != core)
            def _():
                send_ref[0, to] = part


def weight_kernel(where_ref, mine_ref, early_ref, one_ref, two_ref, three_ref, *refs):
    core = where_ref[0, 0]
    high = where_ref[0, 2]
    at_x = where_ref[0, 3]
    dv_refs, (keep_ref, send_ref, grad_s) = refs[:XS], refs[XS:]
    for i in range(CHIPS):
        slab = 2 * i + high if i < XS else 2 * (at_x ^ (i - XS)) + 1 - high
        for k in range(XS):
            grad_s[i * TOK : (i + 1) * TOK, k * HEAD : (k + 1) * HEAD] = dv_refs[k][slab]
    grads = grad_s[...]

    def rows_of(part, c):
        at = pl.ds(pl.multiple_of(part * 2 * ROWS + c * ROWS, 32), ROWS)
        tokens = [mine_ref[i, at, :] for i in range(XS)]
        tokens += [early_ref[0, at, :]] + [ref[at, :] for ref in (one_ref, two_ref, three_ref)]
        return dot(jnp.concatenate(tokens, axis=1), grads, ((1,), (0,)))

    for part in range(2):
        mine = rows_of(part, core).astype(bf16)
        for k in range(XS):
            for r in range(4):
                keep_ref[r, at_x ^ k, part] = mine[r * QUARTER : (r + 1) * QUARTER, k * HEAD : (k + 1) * HEAD]
        sent = rows_of(part, 1 - core).astype(bf16)
        for k in range(XS):
            for r in range(4):
                send_ref[r, at_x ^ k, part] = sent[r * QUARTER : (r + 1) * QUARTER, k * HEAD : (k + 1) * HEAD]


def join_kernel(q_ref, k_ref, came_ref, *out_refs):
    for k in range(CHIPS):
        out_refs[k][0] = q_ref[k]
        out_refs[k][1] = came_ref[0, k]
        out_refs[k][2] = (k_ref[k].astype(f32) + came_ref[1, k].astype(f32)).astype(bf16)


def place_query_kernel(where_ref, *refs):
    core = where_ref[0, 0]
    chip = where_ref[0, 1]
    for k in range(CHIPS):
        head = chip ^ k
        refs[CHIPS][:, block_at(2 * head + core, HEAD)] = refs[k][0]
        refs[CHIPS][:, block_at(2 * head + 1 - core, HEAD)] = refs[k][1]


def place_key_kernel(where_ref, *refs):
    for k in range(CHIPS):
        refs[CHIPS][:, block_at(where_ref[0, 1] ^ k, HEAD)] = refs[k][2]


VMEM = pl.BlockSpec(memory_space=pltpu.VMEM)
SMEM = pl.BlockSpec(memory_space=pltpu.SMEM)
TOKENS = (CHIPS, TOK, HEAD)


def shaped(shape, dtype):
    return jax.ShapeDtypeStruct(shape, dtype)


def call(kernel, specs, outs, scratch=(), flops=10**6, moved=10**6, **more):
    return pl.pallas_call(
        kernel,
        in_specs=specs,
        out_shape=outs,
        scratch_shapes=list(scratch),
        cost_estimate=pl.CostEstimate(flops=flops, bytes_accessed=moved, transcendentals=0),
        **({"out_specs": [VMEM] * len(outs)} | more),
    )


SORTED = [pltpu.VMEM((LENGTH, HEAD), bf16)] * 4
ROWED = [pltpu.VMEM((SLABS, 8, TOK), f32)]
PLACES = [pltpu.SMEM((SLABS,), jnp.int32)]
BLOCK = [pltpu.VMEM((BK, HEAD), f32)]
SEQ = ("x", "yh", "core")
SWAP = [(0, 1), (1, 0)]


def swapped(array, axis="core"):
    return lax.ppermute(array, axis, SWAP)


def along_x(array, k):
    return lax.ppermute(array, "x", [(i, i ^ k) for i in range(XS)])


def inner(
    query_rows, key_rows, value_rows, attn_output, output_grad, log_norm, slab_order, normed_input
):
    core, high, at_x = (lax.axis_index(a).astype(jnp.int32) for a in ("core", "yh", "x"))
    where = jnp.stack([core, at_x * 2 + high, high, at_x]).reshape(1, 4)
    wide = pl.BlockSpec((TOK, PACKED * HEAD), lambda i: (0, i))
    narrow = pl.BlockSpec((TOK, PACKED // 2 * HEAD), lambda i: (0, i))
    (packed,) = call(
        pack_kernel, [SMEM, wide, wide, wide, narrow, narrow, VMEM], [shaped((SLABS, PACK, HEAD), bf16)],
        grid=(SLABS // PACKED,), out_specs=[pl.BlockSpec((PACKED, PACK, HEAD), lambda i: (i, 0, 0))],
    )(
        slab_order, query_rows[0], output_grad[0], attn_output[0], key_rows[0], value_rows[0], log_norm[0]
    )
    got = lax.all_to_all(packed, SEQ, 0, 0, tiled=True)
    (early,) = call(
        pack_early_kernel, [SMEM, VMEM], [shaped((len(EARLY), TILES * TOK, 128), bf16)]
    )(where, normed_input[0])
    (late,) = call(pack_late_kernel, [VMEM], [shaped((XS, TILES * TOK, 128), bf16)])(normed_input[0])
    early = swapped(early, "yh")
    got, late = lax.optimization_barrier((got, late))
    other = swapped(got[:, 2 * TOK : 3 * TOK, :])
    late = lax.all_to_all(late, "x", 0, 0, tiled=True)
    v_keep, v_send, q_keep, k_keep, qk_send = call(
        attn_kernel, [SMEM, VMEM, VMEM],
        [shaped(TOKENS, bf16)] * 4 + [shaped((2, *TOKENS), bf16)],
        SORTED + ROWED + [pltpu.VMEM((LENGTH // BQ, HEAD, BQ), f32)] + BLOCK * 2 + PLACES,
        flops=6 * 10**9,
    )(where, got, other)
    v_came = swapped(v_send)
    dv = (v_keep.astype(f32) + v_came.astype(f32)).astype(bf16)
    dvs = [dv]
    for k in range(1, XS):
        dvs.append(along_x(dv, k))
    two = swapped(lax.dynamic_index_in_dim(late, at_x ^ 2, 0, False), "yh")
    one, three = along_x(early[1], 1), along_x(early[2], 3)
    qk_came = swapped(qk_send)
    w_shape = (4, XS, 2, QUARTER, HEAD)
    w_keep, w_send = call(
        weight_kernel, [SMEM] + [VMEM] * (5 + XS),
        [shaped(w_shape, bf16)] * 2,
        [pltpu.VMEM((LENGTH // 2, XS * HEAD), bf16)], flops=2 * 10**9,
    )(where, late, early, one, two, three, *dvs)
    w_came = swapped(w_send)
    w = (w_keep.astype(f32) + w_came.astype(f32)).astype(bf16)
    parts = lax.all_to_all(w.reshape(SLABS, 2 * QUARTER, HEAD), "batch", 0, 0, tiled=True)
    back = call(join_kernel, [VMEM] * 3, [shaped((3, TOK, HEAD), bf16)] * CHIPS)(
        q_keep, k_keep, qk_came
    )
    pieces = [back[0]]
    for k in range(1, CHIPS):
        pieces.append(lax.ppermute(back[k], SEQ, [(i, i ^ (2 * k)) for i in range(SLABS)]))
    piece = jnp.sum(parts.astype(f32), axis=0).astype(bf16).reshape(1, 2, QUARTER, HEAD)
    blocks = lax.all_to_all(
        jnp.broadcast_to(piece, (SLABS, 2, QUARTER, HEAD)).reshape(2 * SLABS, QUARTER, HEAD),
        ("batch", "yh"), 0, 0, tiled=True,
    )
    (grad_query,) = call(
        place_query_kernel, [SMEM] + [VMEM] * CHIPS, [shaped((TOK, HEADS * HEAD), bf16)]
    )(where, *pieces)
    (grad_key,) = call(
        place_key_kernel, [SMEM] + [VMEM] * CHIPS, [shaped((TOK, KV_HEADS * HEAD), bf16)]
    )(where, *pieces)
    weight = blocks.reshape(4, KV_HEADS, QUARTER, HEAD).transpose(0, 2, 1, 3).reshape(ROWS, KV_HEADS * HEAD)
    return (grad_query[None], grad_key[None], weight.astype(f32))


def solution(mesh):
    fine = Mesh(mesh.devices.reshape(4, 2, 2, 16), (*SEQ, "batch"))
    rows = P("batch", SEQ, None)
    return jax.shard_map(
        inner,
        mesh=fine,
        in_specs=(rows, rows, rows, rows, rows, P("batch", None, SEQ), P("batch", SEQ), rows),
        out_specs=(rows, rows, P(SEQ, None)),
        check_vma=False,
    )
```

```python
import functools

import jax
import jax.numpy as jnp
from jax import lax
from jax.experimental import pallas as pl
from jax.experimental.pallas import tpu as pltpu
from jax.sharding import Mesh, PartitionSpec as P


HEADS = 16
KV_HEADS = 8
HEAD = 128
TOK = 128
SLABS = 16
LENGTH = 2048
CHIPS = 8
D = 4608
ROWS = D // SLABS
QUARTER = ROWS // 4
BK = 512
BQ = 512
HALF = TOK // 2
PACK = 3 * TOK + 8
TILES = 9
XS = 4

SCALE = 144.0 ** (-0.5)
LOG2E = 1.4426950408889634

f32 = jnp.float32
bf16 = jnp.bfloat16


def dot(a, b, dims):
    return lax.dot_general(a, b, (dims, ((), ())), preferred_element_type=f32)


def three_parts(x):
    hi = x.astype(bf16).astype(f32)
    rest = x - hi
    mid = rest.astype(bf16).astype(f32)
    low = (rest - mid).astype(bf16).astype(f32)
    return hi, mid, low


def pack_kernel(place_ref, q_ref, g_ref, o_ref, k_ref, v_ref, n_ref, out_ref):
    place = jnp.full((1, TOK), place_ref[0, 0], jnp.int32).astype(f32)
    for s in range(SLABS):
        cols = slice(s * HEAD, (s + 1) * HEAD)
        kv_cols = slice((s // 2) * HEAD, (s // 2 + 1) * HEAD)
        half = slice((s % 2) * HALF, (s % 2 + 1) * HALF)
        grads = g_ref[:, cols]
        out_ref[s, 0:TOK, :] = q_ref[:, cols]
        out_ref[s, TOK : 2 * TOK, :] = grads
        out_ref[s, 2 * TOK : 2 * TOK + HALF, :] = k_ref[half, kv_cols]
        out_ref[s, 2 * TOK + HALF : 3 * TOK, :] = v_ref[half, kv_cols]
        prod = grads.astype(f32) * o_ref[:, cols].astype(f32)
        delta = jnp.sum(prod.T, axis=0, keepdims=True)
        rows = (*three_parts(n_ref[s : s + 1, :]), *three_parts(delta), place, jnp.zeros_like(place))
        out_ref[s, 3 * TOK :, :] = jnp.concatenate(rows, axis=0).astype(bf16)


def turn_kernel(ks, where_ref, x_ref, *out_refs):
    for k, out_ref in zip(ks, out_refs):
        for t in range(TILES):
            tile = (where_ref[0, 3] ^ k) * TILES + t
            out_ref[t * TOK : (t + 1) * TOK, :] = x_ref[:, block_at(tile, 128)].T


def sort_slabs(core, in_ref, oth_ref, q_s, g_s, k_s, v_s, nd_s, inv_s):
    places = [jnp.max(in_ref[s, 3 * TOK :, :].astype(f32)[6:7, :]).astype(jnp.int32) for s in range(SLABS)]
    for s, p in enumerate(places):
        extra = in_ref[s, 3 * TOK :, :].astype(f32)
        inv_s[p] = s
        at = pl.ds(pl.multiple_of(p * TOK, TOK), TOK)
        q_s[at, :] = in_ref[s, 0:TOK, :]
        g_s[at, :] = in_ref[s, TOK : 2 * TOK, :]
        low = pl.ds(pl.multiple_of(p * TOK, TOK), HALF)
        high = pl.ds(pl.multiple_of(p * TOK + HALF, HALF), HALF)
        for part, out in enumerate((k_s, v_s)):
            own = in_ref[s, 2 * TOK + part * HALF : 2 * TOK + (part + 1) * HALF, :]
            oth = oth_ref[s, part * HALF : (part + 1) * HALF, :]
            out[low, :] = jnp.where(core == 0, own, oth)
            out[high, :] = jnp.where(core == 0, oth, own)
        nd_s[p, 0:1, :] = (extra[0:1] + extra[1:2] + extra[2:3]) * LOG2E
        nd_s[p, 1:2, :] = extra[3:4] + extra[4:5] + extra[5:6]


def row_of(nd_s, i, row):
    return jnp.concatenate([nd_s[i * (BQ // TOK) + t, row : row + 1, :] for t in range(BQ // TOK)], axis=1)


def block_at(i, size):
    if isinstance(i, int):
        return pl.ds(i * size, size)
    return pl.ds(pl.multiple_of(i * size, size), size)


def attn_kernel(
    where_ref, in_ref, oth_ref, vkeep_ref, vsend_ref, qkeep_ref, kkeep_ref, send_ref,
    q_s, g_s, k_s, v_s, nd_s, dq_s, dk_s, dv_s, inv_s,
):
    core = where_ref[0, 0]
    chip = where_ref[0, 1]
    sort_slabs(core, in_ref, oth_ref, q_s, g_s, k_s, v_s, nd_s, inv_s)
    dq_s[...] = jnp.zeros_like(dq_s)

    def per_key_block(j):
        kb = k_s[block_at(j, BK), :]
        vb = v_s[block_at(j, BK), :]
        kt = kb.T
        first = j // (BQ // BK)

        def one(i, masked):
            qb = q_s[block_at(i, BQ), :]
            gb = g_s[block_at(i, BQ), :]
            st = dot(kb, qb, ((1,), (1,)))
            probs = jnp.exp2(st * (SCALE * LOG2E) - row_of(nd_s, i, 0))
            if masked:
                key_at = lax.broadcasted_iota(jnp.int32, (BK, BQ), 0) + j * BK
                query_at = lax.broadcasted_iota(jnp.int32, (BK, BQ), 1) + i * BQ
                probs = jnp.where(key_at <= query_at, probs, 0.0)
            dprob = dot(vb, gb, ((1,), (1,)))
            ds = (probs * (dprob - row_of(nd_s, i, 1))).astype(bf16)
            dv = dot(probs.astype(bf16), gb, ((1,), (0,)))
            dk = dot(ds, qb, ((1,), (0,)))
            dq_s[i] += dot(kt, ds, ((1,), (0,)))
            return dk, dv

        dk_s[...], dv_s[...] = one(first, True)

        def per_query_block(i):
            dk, dv = one(i, False)
            dk_s[...] += dk
            dv_s[...] += dv
            return 0

        for i in range(first + 1, LENGTH // BQ):
            per_query_block(i)
        for t in range(BK // TOK):
            s = inv_s[j * (BK // TOK) + t]
            to = (s // 2) ^ chip
            rows = slice(t * TOK, (t + 1) * TOK)

            @pl.when(s % 2 == core)
            def _():
                vkeep_ref[s // 2] = dv_s[rows, :].astype(bf16)
                kkeep_ref[to] = (dk_s[rows, :] * SCALE).astype(bf16)

            @pl.when(s % 2 != core)
            def _():
                vsend_ref[s // 2] = dv_s[rows, :].astype(bf16)
                send_ref[1, to] = (dk_s[rows, :] * SCALE).astype(bf16)

        return 0

    for j in range(LENGTH // BK):
        per_key_block(j)
    for i in range(LENGTH // BQ):
        rows = (dq_s[i].T * SCALE).astype(bf16)
        for t in range(BQ // TOK):
            s = inv_s[i * (BQ // TOK) + t]
            to = (s // 2) ^ chip
            part = rows[t * TOK : (t + 1) * TOK, :]

            @pl.when(s % 2 == core)
            def _():
                qkeep_ref[to] = part

            @pl.when(s % 2 != core)
            def _():
                send_ref[0, to] = part


def weight_kernel(where_ref, *refs):
    core = where_ref[0, 0]
    high = where_ref[0, 2]
    at_x = where_ref[0, 3]
    x_refs, dv_refs, (keep_ref, send_ref, grad_s) = refs[: 2 * XS], refs[2 * XS : 3 * XS], refs[3 * XS :]
    for i in range(2 * XS):
        slab = 2 * (at_x ^ (i % XS)) + (high if i < XS else 1 - high)
        for k in range(XS):
            grad_s[i * TOK : (i + 1) * TOK, k * HEAD : (k + 1) * HEAD] = dv_refs[k][slab]
    grads = grad_s[...]

    def rows_of(part, c):
        at = pl.ds(pl.multiple_of(part * 2 * ROWS + c * ROWS, 32), ROWS)
        tokens = [ref[at, :] for ref in x_refs]
        return dot(jnp.concatenate(tokens, axis=1), grads, ((1,), (0,)))

    for part in range(2):
        mine = rows_of(part, core).astype(bf16)
        for k in range(XS):
            for r in range(4):
                keep_ref[r, at_x ^ k, part] = mine[r * QUARTER : (r + 1) * QUARTER, k * HEAD : (k + 1) * HEAD]
        sent = rows_of(part, 1 - core).astype(bf16)
        for k in range(XS):
            for r in range(4):
                send_ref[r, at_x ^ k, part] = sent[r * QUARTER : (r + 1) * QUARTER, k * HEAD : (k + 1) * HEAD]


def join_kernel(q_ref, k_ref, came_ref, *out_refs):
    for k in range(CHIPS):
        out_refs[k][0] = q_ref[k]
        out_refs[k][1] = came_ref[0, k]
        out_refs[k][2] = (k_ref[k].astype(f32) + came_ref[1, k].astype(f32)).astype(bf16)


def place_query_kernel(where_ref, *refs):
    core = where_ref[0, 0]
    chip = where_ref[0, 1]
    for k in range(CHIPS):
        head = chip ^ k
        refs[CHIPS][:, block_at(2 * head + core, HEAD)] = refs[k][0]
        refs[CHIPS][:, block_at(2 * head + 1 - core, HEAD)] = refs[k][1]


def place_key_kernel(where_ref, *refs):
    for k in range(CHIPS):
        refs[CHIPS][:, block_at(where_ref[0, 1] ^ k, HEAD)] = refs[k][2]


VMEM = pl.BlockSpec(memory_space=pltpu.VMEM)
SMEM = pl.BlockSpec(memory_space=pltpu.SMEM)
TOKENS = (CHIPS, TOK, HEAD)


def shaped(shape, dtype):
    return jax.ShapeDtypeStruct(shape, dtype)


def call(kernel, specs, outs, scratch=(), flops=10**6, moved=10**6, **more):
    return pl.pallas_call(
        kernel,
        in_specs=specs,
        out_shape=outs,
        scratch_shapes=list(scratch),
        cost_estimate=pl.CostEstimate(flops=flops, bytes_accessed=moved, transcendentals=0),
        **({"out_specs": [VMEM] * len(outs)} | more),
    )


SORTED = [pltpu.VMEM((LENGTH, HEAD), bf16)] * 4
ROWED = [pltpu.VMEM((SLABS, 8, TOK), f32)]
PLACES = [pltpu.SMEM((SLABS,), jnp.int32)]
BLOCK = [pltpu.VMEM((BK, HEAD), f32)]
SEQ = ("x", "yh", "core")
SWAP = [(0, 1), (1, 0)]


def swapped(array, axis="core"):
    return lax.ppermute(array, axis, SWAP)


def along_x(array, k):
    return lax.ppermute(array, "x", [(i, i ^ k) for i in range(XS)])


def inner(
    query_rows, key_rows, value_rows, attn_output, output_grad, log_norm, slab_order, normed_input
):
    core, high, at_x = (lax.axis_index(a).astype(jnp.int32) for a in ("core", "yh", "x"))
    where = jnp.stack([core, at_x * 2 + high, high, at_x]).reshape(1, 4)
    (packed,) = call(pack_kernel, [SMEM] + [VMEM] * 6, [shaped((SLABS, PACK, HEAD), bf16)])(
        slab_order, query_rows[0], output_grad[0], attn_output[0], key_rows[0], value_rows[0], log_norm[0]
    )
    got = lax.all_to_all(packed, SEQ, 0, 0, tiled=True)

    def turned(*ks):
        return call(
            functools.partial(turn_kernel, ks), [SMEM, VMEM], [shaped((TILES * TOK, 128), bf16)] * len(ks)
        )(where, normed_input[0])

    near = turned(0, 1)
    near = [swapped(block, "yh") for block in near]
    far = turned(1, 2, 3)
    mine = [along_x(block, k) for k, block in zip((1, 2, 3), far)]
    mine = [*turned(0), *mine]
    other = swapped(got[:, 2 * TOK : 3 * TOK, :])
    v_keep, v_send, q_keep, k_keep, qk_send = call(
        attn_kernel, [SMEM, VMEM, VMEM],
        [shaped(TOKENS, bf16)] * 4 + [shaped((2, *TOKENS), bf16)],
        SORTED + ROWED + [pltpu.VMEM((LENGTH // BQ, HEAD, BQ), f32)] + BLOCK * 2 + PLACES,
        flops=6 * 10**9,
    )(where, got, other)
    v_came = swapped(v_send)
    dv = (v_keep.astype(f32) + v_came.astype(f32)).astype(bf16)
    dvs = [dv]
    for k in range(1, XS):
        dvs.append(along_x(dv, k))
    crossed = [swapped(mine[k], "yh") for k in (2, 3)]
    crossed = [near[0], along_x(near[1], 1), *crossed]
    qk_came = swapped(qk_send)
    w_shape = (4, XS, 2, QUARTER, HEAD)
    w_keep, w_send = call(
        weight_kernel, [SMEM] + [VMEM] * (3 * XS),
        [shaped(w_shape, bf16)] * 2,
        [pltpu.VMEM((LENGTH // 2, XS * HEAD), bf16)], flops=2 * 10**9,
    )(where, *mine, *crossed, *dvs)
    w_came = swapped(w_send)
    w = (w_keep.astype(f32) + w_came.astype(f32)).astype(bf16)
    parts = lax.all_to_all(w.reshape(SLABS, 2 * QUARTER, HEAD), "batch", 0, 0, tiled=True)
    back = call(join_kernel, [VMEM] * 3, [shaped((3, TOK, HEAD), bf16)] * CHIPS)(
        q_keep, k_keep, qk_came
    )
    pieces = [back[0]]
    for k in range(1, CHIPS):
        pieces.append(lax.ppermute(back[k], SEQ, [(i, i ^ (2 * k)) for i in range(SLABS)]))
    piece = jnp.sum(parts.astype(f32), axis=0).astype(bf16).reshape(1, 2, QUARTER, HEAD)
    blocks = lax.all_to_all(
        jnp.broadcast_to(piece, (SLABS, 2, QUARTER, HEAD)).reshape(2 * SLABS, QUARTER, HEAD),
        ("batch", "yh"), 0, 0, tiled=True,
    )
    (grad_query,) = call(
        place_query_kernel, [SMEM] + [VMEM] * CHIPS, [shaped((TOK, HEADS * HEAD), bf16)]
    )(where, *pieces)
    (grad_key,) = call(
        place_key_kernel, [SMEM] + [VMEM] * CHIPS, [shaped((TOK, KV_HEADS * HEAD), bf16)]
    )(where, *pieces)
    weight = blocks.reshape(4, KV_HEADS, QUARTER, HEAD).transpose(0, 2, 1, 3).reshape(ROWS, KV_HEADS * HEAD)
    return (grad_query[None], grad_key[None], weight.astype(f32))


def solution(mesh):
    fine = Mesh(mesh.devices.reshape(4, 2, 2, 16), (*SEQ, "batch"))
    rows = P("batch", SEQ, None)
    return jax.shard_map(
        inner,
        mesh=fine,
        in_specs=(rows, rows, rows, rows, rows, P("batch", None, SEQ), P("batch", SEQ), rows),
        out_specs=(rows, rows, P(SEQ, None)),
        check_vma=False,
    )
```
